256 devices in a mesh: gx: 16 (over y, x), gy: 16 (over z, core).
Axes of the slice: x: 4, y: 4, z: 8, core: 2. Of those that a mesh axis runs over, the one named last changes fastest.
Arguments:
- background: bfloat16 [40, 256, 512, 128], P(None, 'gx', 'gy'), may hold values from -6 to 6
- obs_perturb: bfloat16 [16, 16, 40, 256], P('gx', 'gy'), may hold values from -1.796875 to 1.796875
- innovation: float32 [16, 16, 256], P('gx', 'gy'), may hold values from -3.8 to 3.8
- obs_precision: float32 [16, 16, 256], P('gx', 'gy'), may hold values from 0.3 to 3
- obs_column: int32 [16, 16, 256], P('gx', 'gy'), may hold values from 0 to 511
- obs_count: int32 [16, 16], P('gx', 'gy'), may hold values from 64 to 256, as said below
Outputs:
- analysis: bfloat16 [40, 256, 512, 128], P(None, 'gx', 'gy')
The draws below stay inside these ranges and needn't reach their ends.
Inputs may be any that keep to these rules, and one draw needn't show every extreme that they name: Slots 0 to obs_count - 1 of a tile hold observations, the others are padding; in every draw some tile has all 256 slots live.
All inputs are finite; a program needn't handle non-finite values.
Results may differ from the reference program's by a relative error of at most 0.001.
Values sent between devices are 32-bit elements; how exact they have to be, the bound alone decides.
A program may use at most 128 MiB of HBM per device.

```python
import math
import jax
import jax.numpy as jnp
from jax import lax

MEMBERS = 40
LEV = 128
OBS_SLOTS_TILE = 256
RX = 8
RY = 16
SPAN = 2
TILES_X = 16
TILES_Y = 16
CX = 16
CY = 32
NX = 256
NY = 512
N_GX = 16
N_GY = 16


def draw_innovation(key, part):
    extent = (TILES_X, TILES_Y, OBS_SLOTS_TILE)
    rising = 1.0 + 2.0 * jnp.arange(TILES_Y, dtype=jnp.float32) / (TILES_Y - 1)
    jitter = jnp.clip(jax.random.normal(key, extent, jnp.float32), -4.0, 4.0)
    tilted = jnp.ones((TILES_X,), jnp.float32)
    return 0.3 * rising[None, :, None] * tilted[:, None, None] * jitter


def draw_obs_count(key, part):
    counts = jax.random.randint(jax.random.fold_in(key, 11), (TILES_X, TILES_Y), OBS_SLOTS_TILE // 4, OBS_SLOTS_TILE + 1)
    selected_entry = jax.random.randint(jax.random.fold_in(key, 12), (), 0, TILES_X * TILES_Y)
    places = jnp.arange(TILES_X * TILES_Y).reshape(TILES_X, TILES_Y)
    return jnp.where(places == selected_entry, OBS_SLOTS_TILE, counts).astype(jnp.int32)


def place_ends(values, key, low, largest):
    shape = values.shape
    place = [jax.random.randint(jax.random.fold_in(key, axis), (), 0, shape[axis]) for axis in range(len(shape))]
    values = values.at[tuple(place)].set(low)
    longest = shape.index(max(shape))
    place[longest] = (place[longest] + 1) % shape[longest]
    return values.at[tuple(place)].set(largest)


def block_levels(own_key, shape, shards, least, largest):
    level, own = 1.0, jax.random.fold_in(own_key, 6)
    for dim, parts in shards:
        draws = jnp.exp(jax.random.uniform(jax.random.fold_in(own, dim), (parts,), jnp.float32, least / len(shards), largest / len(shards)))
        level = level * jnp.repeat(draws, shape[dim] // parts).reshape([-1 if axis == dim else 1 for axis in range(len(shape))])
    return level


def centred(rng, shape, scale, most, shards=(), kind=jnp.bfloat16):
    drawn = scale * jax.random.normal(rng, shape, jnp.float32)
    if shards:
        drawn = drawn * block_levels(rng, shape, shards, -0.22, 0.18)
    return jnp.clip(drawn, -most, most).astype(kind)


def setup_inputs(seed: int = 0) -> dict:
    key_list = jax.random.split(jax.random.key(seed), 7)
    background = centred(key_list[0], (MEMBERS, NX, NY, LEV), 1.0, 6.0, ((1, 16), (2, 16)))
    obs_perturb = centred(key_list[1], (TILES_X, TILES_Y, MEMBERS, OBS_SLOTS_TILE), 0.3, 1.796875, ((0, 16), (1, 16)))
    innovation = draw_innovation(jax.random.fold_in(key_list[6], 71), 0)
    obs_precision = jnp.clip(jnp.exp(math.log(3.0) - 2.3025851 * jax.random.uniform(key_list[3], (TILES_X, TILES_Y, OBS_SLOTS_TILE), jnp.float32) ** block_levels(key_list[3], (TILES_X, TILES_Y, OBS_SLOTS_TILE), ((0, 16), (1, 16)), -0.2, 0.2)), 0.3, 3.0)
    obs_column = place_ends(jax.random.randint(key_list[4], (TILES_X, TILES_Y, OBS_SLOTS_TILE), 0, CX * CY), jax.random.fold_in(key_list[4], 1), 0, (CX * CY) - 1).astype(jnp.int32)
    obs_count = draw_obs_count(jax.random.fold_in(key_list[6], 71), 0)
    return {"background": background, "obs_perturb": obs_perturb, "innovation": innovation, "obs_precision": obs_precision, "obs_column": obs_column, "obs_count": obs_count}


def pair_table(centered, values):
    members = centered.shape[0]
    squares = (centered[:, None, :] * centered[None, :, :]).reshape(members * members, centered.shape[1])
    return jnp.concatenate([squares, centered * values[None, :]], axis=0)

def taper(east_pos, north_pos, centre_east, centre_north, period, radius):
    offset_east = jnp.mod(east_pos[:, None] - centre_east[None, :] + 0.5 * period, period) - 0.5 * period
    offset_north = north_pos[:, None] - centre_north[None, :]
    ratio = (offset_east * offset_east + offset_north * offset_north) / (radius * radius)
    return jnp.square(jnp.maximum(1.0 - ratio, 0.0))

def region_centres(tile_east, northward_tile, count_east, count_north, span, width_east, width_north):
    rows_east = (jnp.arange(count_east) * span).astype(jnp.float32) + 0.5 * span
    rows_north = (jnp.arange(count_north) * span).astype(jnp.float32) + 0.5 * span
    base_east = (tile_east * width_east).astype(jnp.float32)
    base_north = (northward_tile * width_north).astype(jnp.float32)
    centre_east = jnp.broadcast_to(base_east + rows_east[:, None], (count_east, count_north)).reshape(-1)
    centre_north = jnp.broadcast_to(base_north + rows_north[None, :], (count_east, count_north)).reshape(-1)
    return (centre_east, centre_north)

def chol_lower(system):
    members = system.shape[0]
    rows = jnp.arange(members)
    remain = system
    columns = []
    for pivot_id in range(members):
        pivot = jnp.sqrt(remain[pivot_id, pivot_id])
        column = jnp.where((rows >= pivot_id)[:, None], remain[:, pivot_id] / pivot[None, :], 0.0)
        columns.append(column)
        remain = remain - column[:, None, :] * column[None, :, :]
    return jnp.stack(columns, axis=1)

def lower_inverse(factor):
    members = factor.shape[0]
    remain = jnp.broadcast_to(jnp.eye(members, dtype=factor.dtype)[:, :, None], factor.shape)
    solved = []
    for pivot_id in range(members):
        row_now = remain[pivot_id] / factor[pivot_id, pivot_id][None, :]
        solved.append(row_now)
        remain = remain - factor[:, pivot_id][:, None, :] * row_now[None, :, :]
    return jnp.stack(solved, axis=0)

def transform_of(gram, prior_term, members):
    square = members * members
    system = gram[:square].reshape(members, members, -1) + prior_term * jnp.eye(members, dtype=gram.dtype)[:, :, None]
    pull = gram[square:]
    inverse = lower_inverse(chol_lower(system))
    inner = jnp.einsum('imr,mr->ir', inverse, pull, precision=lax.Precision.HIGHEST)
    mean_weights = jnp.einsum('imr,ir->mr', inverse, inner, precision=lax.Precision.HIGHEST)
    return mean_weights[:, None, :] + math.sqrt(members - 1) * jnp.transpose(inverse, (1, 0, 2))

def interp_matrix(columns, regions, span):
    position = jnp.arange(columns).astype(jnp.float32) + 0.5
    centre = (jnp.arange(regions + 2) - 1).astype(jnp.float32) * span + 0.5 * span
    return jnp.maximum(1.0 - jnp.abs(position[:, None] - centre[None, :]) / span, 0.0)

def apply_tile(state_tile, local_frame, span):
    members, cols_east, cols_north, levels = state_tile.shape
    interpolation_rows = interp_matrix(cols_east, local_frame.shape[0] - 2, span)
    interp_cols = interp_matrix(cols_north, local_frame.shape[1] - 2, span)
    halfway_result = jnp.einsum('br,rjg->bjg', interpolation_rows, local_frame, precision=lax.Precision.HIGHEST)
    column_transform = jnp.einsum('bq,aqm->abm', interp_cols, halfway_result, precision=lax.Precision.HIGHEST)
    column_transform = column_transform.reshape(cols_east, cols_north, members, members)
    float_state = state_tile.astype(jnp.float32)
    centre_mean = lax.optimization_barrier(jnp.mean(float_state, axis=0))
    spread = float_state - centre_mean[None]
    update = jnp.einsum('jabl,abjk->kabl', spread, column_transform, precision=lax.Precision.HIGHEST)
    return (centre_mean[None] + update).astype(jnp.bfloat16)

def reference(background, obs_perturb, innovation, obs_precision, obs_column, obs_count):
    members = MEMBERS
    square = members * members
    centered = obs_perturb.astype(jnp.float32)
    centered = centered - lax.optimization_barrier(jnp.mean(centered, axis=2, keepdims=True))
    slots = jnp.arange(OBS_SLOTS_TILE, dtype=jnp.int32)
    live = (slots[None, None, :] < obs_count[:, :, None]).astype(jnp.float32)
    weight = obs_precision * live
    tiles_east = jnp.arange(N_GX, dtype=jnp.int32)[:, None, None]
    tiles_north = jnp.arange(N_GY, dtype=jnp.int32)[None, :, None]
    east_pos = (tiles_east * CX + obs_column // CY).astype(jnp.float32) + 0.5
    north_pos = (tiles_north * CY + obs_column % CY).astype(jnp.float32) + 0.5
    numer = jnp.sum(weight * innovation * innovation)
    denom = jnp.sum(weight * lax.optimization_barrier(jnp.sum(centered * centered, axis=2))) / (members - 1)
    prior_term = (members - 1) / (numer / denom)
    period = float(NX)
    radius = float(CX)
    zero = jnp.zeros((), jnp.int32)

    def tile_weight_matrix(tile_id):
        tile_east = tile_id // N_GY
        northward_tile = tile_id % N_GY
        centre_east, centre_north = region_centres(tile_east, northward_tile, RX, RY, SPAN, CX, CY)
        gram = jnp.zeros((square + members, RX * RY), jnp.float32)
        for step_east in (-1, 0, 1):
            for step_north in (-1, 0, 1):
                source_east = (tile_east + step_east) % N_GX
                source_north = (northward_tile + step_north) % N_GY
                products = pair_table(centered[source_east, source_north], innovation[source_east, source_north])
                reach = taper(east_pos[source_east, source_north], north_pos[source_east, source_north], centre_east, centre_north, period, radius)
                reach = reach * weight[source_east, source_north][:, None]
                gram = gram + jnp.dot(products, reach, precision=lax.Precision.HIGHEST, preferred_element_type=jnp.float32)
        trans = transform_of(gram, prior_term, members)
        return jnp.transpose(trans, (2, 0, 1)).reshape(RX, RY, square)
    tile_ids = jnp.arange(N_GX * N_GY, dtype=jnp.int32)
    grids = lax.map(tile_weight_matrix, tile_ids)
    grids = grids.reshape(N_GX, N_GY, RX, RY, square).transpose(0, 2, 1, 3, 4).reshape(N_GX * RX, N_GY * RY, square)
    padded = jnp.pad(grids, ((1, 1), (0, 0), (0, 0)), mode='wrap')
    padded = jnp.pad(padded, ((0, 0), (1, 1), (0, 0)), mode='edge')

    def tile_state(tile_id):
        tile_east = tile_id // N_GY
        northward_tile = tile_id % N_GY
        local_frame = lax.dynamic_slice(padded, ((tile_east * RX).astype(jnp.int32), (northward_tile * RY).astype(jnp.int32), zero), (RX + 2, RY + 2, square))
        state_tile = lax.dynamic_slice(background, (zero, (tile_east * CX).astype(jnp.int32), (northward_tile * CY).astype(jnp.int32), zero), (members, CX, CY, LEV))
        return apply_tile(state_tile, local_frame, float(SPAN))
    results = lax.map(tile_state, tile_ids)
    results = results.reshape(N_GX, N_GY, members, CX, CY, LEV).transpose(2, 0, 3, 1, 4, 5)
    return results.reshape(members, NX, NY, LEV)
```

```python
import functools
import math

import jax
import jax.numpy as jnp
from jax import lax
from jax.experimental import pallas as pl
from jax.experimental.pallas import tpu as pltpu
from jax.sharding import PartitionSpec as P

F32 = jnp.float32
BF16 = jnp.bfloat16
MESH = pl.DeviceIdType.MESH
NB = 16
M = 40
SLOTS = 256
CX, CY = 16, 32
RX, RY = 8, 16
NREG = RX * RY
ROWS = 48
GROUPS = 14
STRIDE = 40
NEIGHBOURS = [(-1, -1), (-1, 0), (-1, 1), (0, -1), (0, 1), (1, -1), (1, 0), (1, 1)]


def vmem_specs(count):
    return [pl.BlockSpec(memory_space=pltpu.VMEM)] * count


def exchange_kernel(
    obs_ref, innovation_ref, precision_ref, column_ref, count_ref,
    near_ref, total_ref,
    mine, landed, part_a, part_b, slots_a, slots_b,
    send_near, recv_near, send_a, recv_a, send_b, recv_b,
):
    gx = lax.axis_index("gx")
    gy = lax.axis_index("gy")

    def at(dx, dy):
        return (lax.rem(gx + dx + NB, NB), lax.rem(gy + dy + NB, NB))

    barrier = pltpu.get_barrier_semaphore()
    peers = [(0, d) for d in range(1, NB)] + [(d, 0) for d in range(1, NB)]
    peers += [(1, 1), (1, -1), (-1, 1), (-1, -1)]
    for dx, dy in peers:
        pl.semaphore_signal(barrier, inc=1, device_id=at(dx, dy), device_id_type=MESH)

    centered = obs_ref[...].astype(F32)
    centered = centered - jnp.sum(centered, axis=0, keepdims=True) * (1.0 / M)
    innovation = innovation_ref[...]
    slot = lax.broadcasted_iota(jnp.int32, (1, SLOTS), 1)
    weight = jnp.where(slot < count_ref[...], precision_ref[...], 0.0)
    column = column_ref[...]
    east = (gx * CX + lax.shift_right_logical(column, 5)).astype(F32) + 0.5
    north = (gy * CY + jnp.bitwise_and(column, 31)).astype(F32) + 0.5
    mine[0:M, :] = centered
    mine[M : M + 8, :] = jnp.concatenate(
        [innovation, weight, east, north, jnp.zeros((4, SLOTS), F32)], axis=0
    )
    numer = jnp.sum(weight * innovation * innovation, axis=1, keepdims=True)
    squares = jnp.sum(centered * centered, axis=0, keepdims=True)
    denom = jnp.sum(weight * squares, axis=1, keepdims=True) / (M - 1)
    lane = lax.broadcasted_iota(jnp.int32, (1, 128), 1)
    part = jnp.where(lane < 64, numer, denom)
    part_a[...] = part

    pl.semaphore_wait(barrier, len(peers))

    def spread(src, slots, send, recv, along_x):
        copies = []
        for d in range(1, NB):
            copy = pltpu.make_async_remote_copy(
                src_ref=src,
                dst_ref=slots.at[d],
                send_sem=send.at[d],
                recv_sem=recv.at[d],
                device_id=at(d, 0) if along_x else at(0, d),
                device_id_type=MESH,
            )
            copy.start()
            copies.append(copy)
        return copies

    first = spread(part_a, slots_a, send_a, recv_a, False)
    near = []
    for n, (dx, dy) in enumerate(NEIGHBOURS):
        copy = pltpu.make_async_remote_copy(
            src_ref=mine,
            dst_ref=landed.at[n],
            send_sem=send_near.at[n],
            recv_sem=recv_near.at[n],
            device_id=at(dx, dy),
            device_id_type=MESH,
        )
        copy.start()
        near.append(copy)
    for copy in first:
        copy.wait()
    for d in range(1, NB):
        part = part + slots_a[d]
    part_b[...] = part
    second = spread(part_b, slots_b, send_b, recv_b, True)
    near_ref[0] = mine[...]
    for n, copy in enumerate(near):
        copy.wait()
        near_ref[n + 1] = landed[n]
    for copy in second:
        copy.wait()
    for d in range(1, NB):
        part = part + slots_b[d]
    total_ref[...] = part


def exchange(obs, innovation, precision, column, count):
    return pl.pallas_call(
        exchange_kernel,
        out_shape=(
            jax.ShapeDtypeStruct((9, ROWS, SLOTS), F32),
            jax.ShapeDtypeStruct((1, 128), F32),
        ),
        in_specs=vmem_specs(5),
        out_specs=tuple(vmem_specs(2)),
        scratch_shapes=[
            pltpu.VMEM((ROWS, SLOTS), F32),
            pltpu.VMEM((8, ROWS, SLOTS), F32),
            pltpu.VMEM((1, 128), F32),
            pltpu.VMEM((1, 128), F32),
            pltpu.VMEM((NB, 1, 128), F32),
            pltpu.VMEM((NB, 1, 128), F32),
            pltpu.SemaphoreType.DMA((8,)),
            pltpu.SemaphoreType.DMA((8,)),
            pltpu.SemaphoreType.DMA((NB,)),
            pltpu.SemaphoreType.DMA((NB,)),
            pltpu.SemaphoreType.DMA((NB,)),
            pltpu.SemaphoreType.DMA((NB,)),
        ],
        compiler_params=pltpu.CompilerParams(collective_id=0, has_side_effects=True),
        name="exchange",
    )(obs, innovation, precision, column, count)


BLOCKS = [(ib, jb) for ib in range(5) for jb in range(ib, 5)]


def split(value):
    high = value.astype(BF16)
    return high, (value - high.astype(F32)).astype(BF16)


def solve_kernel(
    near_ref, total_ref, packed_ref, south_ref, north_ref, corner_ref,
    table_high, table_low, gram, upper, inverse, flat,
):
    gx = lax.axis_index("gx")
    gy = lax.axis_index("gy")
    region = lax.broadcasted_iota(jnp.int32, (NREG, SLOTS), 0)
    centre_east = (gx * CX + 2 * lax.shift_right_logical(region, 4)).astype(F32) + 1.0
    centre_north = (gy * CY + 2 * jnp.bitwise_and(region, 15)).astype(F32) + 1.0
    gram[...] = jnp.zeros_like(gram)
    table_high[...] = jnp.zeros_like(table_high)
    table_low[...] = jnp.zeros_like(table_low)

    def tile(t, carry):
        obs = near_ref.at[t]
        east = obs[M + 2 : M + 3, :]
        north = obs[M + 3 : M + 4, :]
        weight = obs[M + 1 : M + 2, :]
        innovation = obs[M : M + 1, :]
        de = east - centre_east + 128.0
        de = jnp.where(de < 0.0, de + 256.0, de)
        de = jnp.where(de >= 256.0, de - 256.0, de) - 128.0
        dn = north - centre_north
        reach = jnp.maximum(1.0 - (de * de + dn * dn) * (1.0 / 256.0), 0.0)
        reach = reach * reach * weight
        reach_high, reach_low = split(reach)
        both = jnp.concatenate([reach_high, reach_low], axis=0)
        for b, (ib, jb) in enumerate(BLOCKS):
            right = obs[8 * jb : 8 * jb + 8, :]
            for ii in range(0, 8, 2):
                i = 8 * ib + ii
                rows = jnp.concatenate(
                    [obs[i : i + 1, :] * right, obs[i + 1 : i + 2, :] * right], axis=0
                )
                high, low = split(rows)
                at = b * 64 + ii * 8
                table_high[at : at + 16, :] = high
                table_low[at : at + 16, :] = low
        pull = jnp.concatenate([obs[0:M, :] * innovation, jnp.zeros((8, SLOTS), F32)], axis=0)
        high, low = split(pull)
        table_high[960:1008, :] = high
        table_low[960:1008, :] = low
        for c in range(0, 1024, 256):
            total = None
            for table in (table_high, table_low):
                out = lax.dot_general(
                    table[c : c + 256, :], both, (((1,), (1,)), ((), ())),
                    preferred_element_type=F32,
                )
                out = out[:, :128] + out[:, 128:]
                total = out if total is None else total + out
            gram[c : c + 256, :] += total
        return carry

    lax.fori_loop(0, 9, tile, 0)

    lane = lax.broadcasted_iota(jnp.int32, (1, 128), 1)
    both = total_ref[...]
    numer = jnp.sum(jnp.where(lane == 0, both, 0.0), axis=1, keepdims=True)
    denom = jnp.sum(jnp.where(lane == 64, both, 0.0), axis=1, keepdims=True)
    prior = jnp.broadcast_to((M - 1) / (numer / denom), (8, 128))
    sub = lax.broadcasted_iota(jnp.int32, (8, 128), 0)
    inverse[...] = jnp.zeros_like(inverse)
    offset = {pair: 64 * b for b, pair in enumerate(BLOCKS)}

    for ib in range(5):
        cols = list(range(ib, 5))
        state = []
        for t in range(8):
            row = []
            for jb in cols:
                at = offset[(ib, jb)] + 8 * t
                value = gram[at : at + 8, :]
                if jb == ib:
                    value = value + jnp.where(sub == t, prior, 0.0)
                row.append(value)
            row += [jnp.zeros((8, 128), F32)] * ib
            state.append(row)

        def eliminate(p, state):
            base = p * M
            line = [upper[pl.ds(pl.multiple_of(base + 8 * jb, 8), 8), :] for jb in cols]
            line += [inverse[pl.ds(pl.multiple_of(base + 8 * jb, 8), 8), :] for jb in range(ib)]
            new = []
            for t in range(8):
                factor = upper[pl.ds(base + 8 * ib + t, 1), :]
                factor = jnp.broadcast_to(factor, (8, 128))
                new.append([s - factor * v for s, v in zip(state[t], line)])
            return new

        if ib:
            state = lax.fori_loop(0, 8 * ib, eliminate, state, unroll=4)
        state = [
            row + [jnp.where(sub == t, 1.0, 0.0).astype(F32)] for t, row in enumerate(state)
        ]
        for t in range(8):
            scale = lax.rsqrt(jnp.broadcast_to(state[t][0][t : t + 1, :], (8, 128)))
            state[t] = [v * scale for v in state[t]]
            for s in range(t + 1, 8):
                factor = jnp.broadcast_to(state[t][0][s : s + 1, :], (8, 128))
                state[s] = [a - factor * v for a, v in zip(state[s], state[t])]
            p = 8 * ib + t
            for jb, value in zip(cols, state[t][: len(cols)]):
                upper[p * M + 8 * jb : p * M + 8 * jb + 8, :] = value
            for jb, value in enumerate(state[t][len(cols) :]):
                inverse[p * M + 8 * jb : p * M + 8 * jb + 8, :] = value

    pull = [gram[960 + 8 * jb : 968 + 8 * jb, :] for jb in range(5)]
    mean = [jnp.zeros((8, 128), F32)] * 5
    sums = []
    for k in range(M):
        rows = [inverse[k * M + 8 * jb : k * M + 8 * jb + 8, :] for jb in range(k // 8 + 1)]
        inner = rows[0] * pull[0]
        plain = rows[0]
        for jb in range(1, len(rows)):
            inner = inner + rows[jb] * pull[jb]
            plain = plain + rows[jb]
        inner = jnp.broadcast_to(jnp.sum(inner, axis=0, keepdims=True), (8, 128))
        sums.append(jnp.broadcast_to(jnp.sum(plain, axis=0, keepdims=True), (8, 128)))
        for jb in range(len(rows)):
            mean[jb] = mean[jb] + rows[jb] * inner
    mean_sum = mean[0] + mean[1] + mean[2] + mean[3] + mean[4]
    mean_sum = jnp.broadcast_to(jnp.sum(mean_sum, axis=0, keepdims=True), (8, 128))
    root = math.sqrt(M - 1)
    for g in range(GROUPS):
        rows = []
        for part in range(3):
            k = part * GROUPS + g
            if k >= M:
                rows += [jnp.zeros((8, 128), F32)] * 5
                continue
            shift = (1.0 - mean_sum - root * sums[k]) * (1.0 / M)
            for jb in range(5):
                value = mean[jb] + shift
                if jb <= k // 8:
                    value = value + root * inverse[k * M + 8 * jb : k * M + 8 * jb + 8, :]
                rows.append(value)
        rows.append(jnp.zeros((8, 128), F32))
        turned = jnp.transpose(jnp.concatenate(rows, axis=0))
        packed_ref[g] = turned
        flat[g * NREG : (g + 1) * NREG, :] = turned
        south_ref[g] = flat[pl.ds(g * NREG, RX, stride=RY), :]
        north_ref[g] = flat[pl.ds(g * NREG + RY - 1, RX, stride=RY), :]
    flat[GROUPS * NREG : 16 * NREG, :] = jnp.zeros((2 * NREG, 128), F32)
    for c, r in enumerate((0, RY - 1, NREG - RY, NREG - 1)):
        corner_ref[c] = flat[pl.ds(r, 16, stride=NREG), :]


def solve(near, total):
    return pl.pallas_call(
        solve_kernel,
        out_shape=(
            jax.ShapeDtypeStruct((GROUPS, NREG, 128), F32),
            jax.ShapeDtypeStruct((GROUPS, RX, 128), F32),
            jax.ShapeDtypeStruct((GROUPS, RX, 128), F32),
            jax.ShapeDtypeStruct((4, 16, 128), F32),
        ),
        in_specs=vmem_specs(2),
        out_specs=tuple(vmem_specs(4)),
        scratch_shapes=[
            pltpu.VMEM((1024, SLOTS), BF16),
            pltpu.VMEM((1024, SLOTS), BF16),
            pltpu.VMEM((1024, NREG), F32),
            pltpu.VMEM((M * M, 128), F32),
            pltpu.VMEM((M * M, 128), F32),
            pltpu.VMEM((16 * NREG, 128), F32),
        ],
        name="solve",
    )(near, total)


def edge_kernel(
    packed_ref, south_ref, north_ref, corner_ref,
    west_out, east_out, south_out, north_out, corner_out,
    west, east, south, north, corner, send, recv,
):
    gx = lax.axis_index("gx")
    gy = lax.axis_index("gy")

    def at(dx, dy):
        return (lax.rem(gx + dx + NB, NB), lax.rem(gy + dy + NB, NB))

    barrier = pltpu.get_barrier_semaphore()
    for dx, dy in NEIGHBOURS:
        pl.semaphore_signal(barrier, inc=1, device_id=at(dx, dy), device_id_type=MESH)
    pl.semaphore_wait(barrier, len(NEIGHBOURS))
    plan = [
        (packed_ref.at[:, pl.ds(0, RY)], east, (-1, 0)),
        (packed_ref.at[:, pl.ds(NREG - RY, RY)], west, (1, 0)),
        (south_ref, north, (0, -1)),
        (north_ref, south, (0, 1)),
        (corner_ref.at[0], corner.at[3], (-1, -1)),
        (corner_ref.at[1], corner.at[2], (-1, 1)),
        (corner_ref.at[2], corner.at[1], (1, -1)),
        (corner_ref.at[3], corner.at[0], (1, 1)),
    ]
    copies = []
    for n, (src, dst, (dx, dy)) in enumerate(plan):
        copy = pltpu.make_async_remote_copy(
            src_ref=src,
            dst_ref=dst,
            send_sem=send.at[n],
            recv_sem=recv.at[n],
            device_id=at(dx, dy),
            device_id_type=MESH,
        )
        copy.start()
        copies.append(copy)
    for copy in copies:
        copy.wait()
    west_out[...] = west[...]
    east_out[...] = east[...]
    south_out[...] = south[...]
    north_out[...] = north[...]
    corner_out[...] = corner[...]


def edges(packed, south, north, corner):
    shapes = [(GROUPS, RY, 128), (GROUPS, RY, 128), (GROUPS, RX, 128), (GROUPS, RX, 128), (4, 16, 128)]
    return pl.pallas_call(
        edge_kernel,
        out_shape=tuple(jax.ShapeDtypeStruct(s, F32) for s in shapes),
        in_specs=vmem_specs(4),
        out_specs=tuple(vmem_specs(5)),
        scratch_shapes=[pltpu.VMEM(s, F32) for s in shapes]
        + [pltpu.SemaphoreType.DMA((8,)), pltpu.SemaphoreType.DMA((8,))],
        compiler_params=pltpu.CompilerParams(collective_id=1, has_side_effects=True),
        name="edges",
    )(packed, south, north, corner)


def apply_kernel(
    state_ref, packed_ref, west_ref, east_ref, south_ref, north_ref, corner_ref,
    out_ref,
    frame, line, weights, members, results,
):
    a = pl.program_id(0)

    @pl.when(a == 0)
    def build():
        gy = lax.axis_index("gy")
        bottom = gy == 0
        top = gy == NB - 1
        for g in range(GROUPS):
            frame[g, 0, 8:24, :] = west_ref[g]
            frame[g, RX + 1, 8:24, :] = east_ref[g]
            frame[g, 0, 7:8, :] = jnp.where(bottom, west_ref[g, 0:1], corner_ref[0, g : g + 1])
            frame[g, 0, 24:25, :] = jnp.where(top, west_ref[g, RY - 1 : RY], corner_ref[1, g : g + 1])
            frame[g, RX + 1, 7:8, :] = jnp.where(bottom, east_ref[g, 0:1], corner_ref[2, g : g + 1])
            frame[g, RX + 1, 24:25, :] = jnp.where(top, east_ref[g, RY - 1 : RY], corner_ref[3, g : g + 1])
            for p in range(RX):
                r = p * RY
                frame[g, p + 1, 8:24, :] = packed_ref[g, r : r + RY, :]
                frame[g, p + 1, 7:8, :] = jnp.where(
                    bottom, packed_ref[g, r : r + 1, :], south_ref[g, p : p + 1]
                )
                frame[g, p + 1, 24:25, :] = jnp.where(
                    top, packed_ref[g, r + RY - 1 : r + RY, :], north_ref[g, p : p + 1]
                )

    p = lax.div(a, 2)
    odd = lax.rem(a, 2)
    for g in range(GROUPS):
        line[...] = 0.75 * frame[g, p + 1] + 0.25 * frame[g, p + 2 * odd]
        centre = 0.75 * line[8:24, :]
        weights[g * STRIDE : g * STRIDE + 16, :] = centre + 0.25 * line[7:23, :]
        weights[g * STRIDE + 16 : g * STRIDE + 32, :] = centre + 0.25 * line[9:25, :]
    for j in range(M):
        members[j * STRIDE : j * STRIDE + CY, :] = state_ref[j, 0].astype(F32)

    lane = lax.broadcasted_iota(jnp.int32, (16, 128), 1)
    low_side = lane >= M

    for y in range(CY):
        q, par = y // 2, y % 2
        block = members[pl.ds(y, M, stride=STRIDE), :].astype(BF16)
        block = jnp.concatenate([block, block], axis=0)
        value = weights[pl.ds(par * 16 + q, 16, stride=STRIDE), :]
        high = value.astype(BF16).astype(F32)
        low = value - high
        low40 = pltpu.roll(low, 128 - 40, 1)
        parts = [
            jnp.where(low_side, pltpu.roll(low, 40, 1), high),
            jnp.where(low_side, low, pltpu.roll(high, 128 - 40, 1)),
            jnp.where(low_side, low40, pltpu.roll(high, 128 - 80, 1)),
        ]
        left = jnp.concatenate([v.astype(BF16) for v in parts], axis=0)[:, : 2 * M]
        out = jnp.dot(left, block, preferred_element_type=F32)
        results[pl.ds(y, 14, stride=STRIDE), :] = out[0:14]
        results[pl.ds(14 * STRIDE + y, 14, stride=STRIDE), :] = out[16:30]
        results[pl.ds(28 * STRIDE + y, 12, stride=STRIDE), :] = out[32:44]
    for k in range(M):
        out_ref[k, 0] = results[k * STRIDE : k * STRIDE + CY, :].astype(BF16)


def apply(state, packed, west, east, south, north, corner):
    def whole(shape):
        return pl.BlockSpec(shape, lambda a: (0,) * len(shape), pipeline_mode=pl.Buffered(1))

    return pl.pallas_call(
        apply_kernel,
        out_shape=jax.ShapeDtypeStruct((M, CX, CY, 128), BF16),
        grid=(CX,),
        in_specs=[
            pl.BlockSpec((M, 1, CY, 128), lambda a: (0, a, 0, 0)),
            whole((GROUPS, NREG, 128)),
            whole((GROUPS, RY, 128)),
            whole((GROUPS, RY, 128)),
            whole((GROUPS, RX, 128)),
            whole((GROUPS, RX, 128)),
            whole((4, 16, 128)),
        ],
        out_specs=pl.BlockSpec((M, 1, CY, 128), lambda a: (0, a, 0, 0)),
        scratch_shapes=[
            pltpu.VMEM((GROUPS, RX + 2, 32, 128), F32),
            pltpu.VMEM((32, 128), F32),
            pltpu.VMEM((16 * STRIDE, 128), F32),
            pltpu.VMEM((M * STRIDE, 128), F32),
            pltpu.VMEM((M * STRIDE, 128), F32),
        ],
        compiler_params=pltpu.CompilerParams(dimension_semantics=("arbitrary",)),
        name="apply",
    )(state, packed, west, east, south, north, corner)


def per_device(background, obs_perturb, innovation, obs_precision, obs_column, obs_count):
    near, total = exchange(
        obs_perturb[0, 0], innovation[0], obs_precision[0], obs_column[0], obs_count
    )
    packed, south, north, corner = solve(near, total)
    west, east, south, north, corner = edges(packed, south, north, corner)
    return apply(background, packed, west, east, south, north, corner)


def solution(mesh):
    return jax.shard_map(
        per_device,
        mesh=mesh,
        in_specs=(
            P(None, "gx", "gy", None),
            P("gx", "gy", None, None),
            P("gx", "gy", None),
            P("gx", "gy", None),
            P("gx", "gy", None),
            P("gx", "gy"),
        ),
        out_specs=P(None, "gx", "gy", None),
        check_vma=False,
    )
```

```python
import functools
import math

import jax
import jax.numpy as jnp
from jax import lax
from jax.experimental import pallas as pl
from jax.experimental.pallas import tpu as pltpu
from jax.sharding import PartitionSpec as P

F32 = jnp.float32
BF16 = jnp.bfloat16
MESH = pl.DeviceIdType.MESH
NB = 16
M = 40
SLOTS = 256
CX, CY = 16, 32
RX, RY = 8, 16
NREG = RX * RY
ROWS = 48
GROUPS = 14
STRIDE = 40
NEIGHBOURS = [(-1, -1), (-1, 0), (-1, 1), (0, -1), (0, 1), (1, -1), (1, 0), (1, 1)]


def vmem_specs(count):
    return [pl.BlockSpec(memory_space=pltpu.VMEM)] * count


BLOCKS = [(ib, jb) for ib in range(5) for jb in range(ib, 5)]


def split(value):
    high = value.astype(BF16)
    return high, (value - high.astype(F32)).astype(BF16)


def analyse_kernel(
    obs_ref, innovation_ref, precision_ref, column_ref, count_ref,
    packed_ref, west_out, east_out, south_out, north_out, corner_out,
    landed, part_a, part_b, slots_a, slots_b,
    table_high, table_low, gram, upper, inverse, flat,
    south_edge, north_edge, corner_edge,
    west_in, east_in, south_in, north_in, corner_in,
    send_near, recv_near, send_a, recv_a, send_b, recv_b, send_edge, recv_edge,
):
    gx = lax.axis_index("gx")
    gy = lax.axis_index("gy")

    def device(dx, dy):
        return (lax.rem(gx + dx + NB, NB), lax.rem(gy + dy + NB, NB))

    barrier = pltpu.get_barrier_semaphore()
    peers = [(0, d) for d in range(1, NB)] + [(d, 0) for d in range(1, NB)]
    peers += [(1, 1), (1, -1), (-1, 1), (-1, -1)]
    for dx, dy in peers:
        pl.semaphore_signal(barrier, inc=1, device_id=device(dx, dy), device_id_type=MESH)

    centered = obs_ref[...].astype(F32)
    centered = centered - jnp.sum(centered, axis=0, keepdims=True) * (1.0 / M)
    innovation = innovation_ref[...]
    slot = lax.broadcasted_iota(jnp.int32, (1, SLOTS), 1)
    weight = jnp.where(slot < count_ref[...], precision_ref[...], 0.0)
    column = column_ref[...]
    east = (gx * CX + lax.shift_right_logical(column, 5)).astype(F32) + 0.5
    north = (gy * CY + jnp.bitwise_and(column, 31)).astype(F32) + 0.5
    mine = landed.at[0]
    mine[0:M, :] = centered
    mine[M : M + 8, :] = jnp.concatenate(
        [innovation, weight, east, north, jnp.zeros((4, SLOTS), F32)], axis=0
    )
    numer = jnp.sum(weight * innovation * innovation, axis=1, keepdims=True)
    squares = jnp.sum(centered * centered, axis=0, keepdims=True)
    denom = jnp.sum(weight * squares, axis=1, keepdims=True) / (M - 1)
    lane = lax.broadcasted_iota(jnp.int32, (1, 128), 1)
    part = jnp.where(lane < 64, numer, denom)
    part_a[...] = part

    pl.semaphore_wait(barrier, len(peers))

    def spread(src, slots, send, recv, along_x):
        copies = []
        for d in range(1, NB):
            copy = pltpu.make_async_remote_copy(
                src_ref=src,
                dst_ref=slots.at[d],
                send_sem=send.at[d],
                recv_sem=recv.at[d],
                device_id=device(d, 0) if along_x else device(0, d),
                device_id_type=MESH,
            )
            copies.append(copy)
        return copies

    first = spread(part_a, slots_a, send_a, recv_a, False)
    for copy in first:
        copy.start()
    near = []
    for n, (dx, dy) in enumerate(NEIGHBOURS):
        copy = pltpu.make_async_remote_copy(
            src_ref=mine,
            dst_ref=landed.at[n + 1],
            send_sem=send_near.at[n],
            recv_sem=recv_near.at[n],
            device_id=device(dx, dy),
            device_id_type=MESH,
        )
        copy.start()
        near.append(copy)
    region = lax.broadcasted_iota(jnp.int32, (NREG, SLOTS), 0)
    centre_east = (gx * CX + 2 * lax.shift_right_logical(region, 4)).astype(F32) + 1.0
    centre_north = (gy * CY + 2 * jnp.bitwise_and(region, 15)).astype(F32) + 1.0
    gram[...] = jnp.zeros_like(gram)
    table_high[...] = jnp.zeros_like(table_high)
    table_low[...] = jnp.zeros_like(table_low)

    def tile(t, carry):
        @pl.when(t == 1)
        def arrive():
            total = part_a[...]
            for copy in first:
                copy.wait()
            for d in range(1, NB):
                total = total + slots_a[d]
            part_b[...] = total
            for copy in spread(part_b, slots_b, send_b, recv_b, True):
                copy.start()
            for copy in near:
                copy.wait()

        obs = landed.at[t]
        east = obs[M + 2 : M + 3, :]
        north = obs[M + 3 : M + 4, :]
        weight = obs[M + 1 : M + 2, :]
        innovation = obs[M : M + 1, :]
        de = east - centre_east + 128.0
        de = jnp.where(de < 0.0, de + 256.0, de)
        de = jnp.where(de >= 256.0, de - 256.0, de) - 128.0
        dn = north - centre_north
        reach = jnp.maximum(1.0 - (de * de + dn * dn) * (1.0 / 256.0), 0.0)
        reach = reach * reach * weight
        reach_high, reach_low = split(reach)
        both = jnp.concatenate([reach_high, reach_low], axis=0)
        for b, (ib, jb) in enumerate(BLOCKS):
            right = obs[8 * jb : 8 * jb + 8, :]
            for ii in range(0, 8, 2):
                i = 8 * ib + ii
                rows = jnp.concatenate(
                    [obs[i : i + 1, :] * right, obs[i + 1 : i + 2, :] * right], axis=0
                )
                high, low = split(rows)
                at = b * 64 + ii * 8
                table_high[at : at + 16, :] = high
                table_low[at : at + 16, :] = low
        pull = jnp.concatenate([obs[0:M, :] * innovation, jnp.zeros((8, SLOTS), F32)], axis=0)
        high, low = split(pull)
        table_high[960:1008, :] = high
        table_low[960:1008, :] = low
        for c in range(0, 1024, 256):
            total = None
            for table in (table_high, table_low):
                out = lax.dot_general(
                    table[c : c + 256, :], both, (((1,), (1,)), ((), ())),
                    preferred_element_type=F32,
                )
                out = out[:, :128] + out[:, 128:]
                total = out if total is None else total + out
            gram[c : c + 256, :] += total
        return carry

    lax.fori_loop(0, 9, tile, 0)

    lane = lax.broadcasted_iota(jnp.int32, (1, 128), 1)
    for copy in spread(part_b, slots_b, send_b, recv_b, True):
        copy.wait()
    both = part_b[...]
    for d in range(1, NB):
        both = both + slots_b[d]
    numer = jnp.sum(jnp.where(lane == 0, both, 0.0), axis=1, keepdims=True)
    denom = jnp.sum(jnp.where(lane == 64, both, 0.0), axis=1, keepdims=True)
    prior = jnp.broadcast_to((M - 1) / (numer / denom), (8, 128))
    sub = lax.broadcasted_iota(jnp.int32, (8, 128), 0)
    inverse[...] = jnp.zeros_like(inverse)
    offset = {pair: 64 * b for b, pair in enumerate(BLOCKS)}

    for ib in range(5):
        cols = list(range(ib, 5))
        state = []
        for t in range(8):
            row = []
            for jb in cols:
                at = offset[(ib, jb)] + 8 * t
                value = gram[at : at + 8, :]
                if jb == ib:
                    value = value + jnp.where(sub == t, prior, 0.0)
                row.append(value)
            row += [jnp.zeros((8, 128), F32)] * ib
            state.append(row)

        def eliminate(p, state):
            base = p * M
            line = [upper[pl.ds(pl.multiple_of(base + 8 * jb, 8), 8), :] for jb in cols]
            line += [inverse[pl.ds(pl.multiple_of(base + 8 * jb, 8), 8), :] for jb in range(ib)]
            new = []
            for t in range(8):
                factor = upper[pl.ds(base + 8 * ib + t, 1), :]
                factor = jnp.broadcast_to(factor, (8, 128))
                new.append([s - factor * v for s, v in zip(state[t], line)])
            return new

        if ib:
            state = lax.fori_loop(0, 8 * ib, eliminate, state, unroll=4)
        state = [
            row + [jnp.where(sub == t, 1.0, 0.0).astype(F32)] for t, row in enumerate(state)
        ]
        for t in range(8):
            scale = lax.rsqrt(jnp.broadcast_to(state[t][0][t : t + 1, :], (8, 128)))
            state[t] = [v * scale for v in state[t]]
            for s in range(t + 1, 8):
                factor = jnp.broadcast_to(state[t][0][s : s + 1, :], (8, 128))
                state[s] = [a - factor * v for a, v in zip(state[s], state[t])]
            p = 8 * ib + t
            for jb, value in zip(cols, state[t][: len(cols)]):
                upper[p * M + 8 * jb : p * M + 8 * jb + 8, :] = value
            for jb, value in enumerate(state[t][len(cols) :]):
                inverse[p * M + 8 * jb : p * M + 8 * jb + 8, :] = value

    pull = [gram[960 + 8 * jb : 968 + 8 * jb, :] for jb in range(5)]
    mean = [jnp.zeros((8, 128), F32)] * 5
    sums = []
    for k in range(M):
        rows = [inverse[k * M + 8 * jb : k * M + 8 * jb + 8, :] for jb in range(k // 8 + 1)]
        inner = rows[0] * pull[0]
        plain = rows[0]
        for jb in range(1, len(rows)):
            inner = inner + rows[jb] * pull[jb]
            plain = plain + rows[jb]
        inner = jnp.broadcast_to(jnp.sum(inner, axis=0, keepdims=True), (8, 128))
        sums.append(jnp.broadcast_to(jnp.sum(plain, axis=0, keepdims=True), (8, 128)))
        for jb in range(len(rows)):
            mean[jb] = mean[jb] + rows[jb] * inner
    mean_sum = mean[0] + mean[1] + mean[2] + mean[3] + mean[4]
    mean_sum = jnp.broadcast_to(jnp.sum(mean_sum, axis=0, keepdims=True), (8, 128))
    root = math.sqrt(M - 1)
    for g in range(GROUPS):
        rows = []
        for part in range(3):
            k = part * GROUPS + g
            if k >= M:
                rows += [jnp.zeros((8, 128), F32)] * 5
                continue
            shift = (1.0 - mean_sum - root * sums[k]) * (1.0 / M)
            for jb in range(5):
                value = mean[jb] + shift
                if jb <= k // 8:
                    value = value + root * inverse[k * M + 8 * jb : k * M + 8 * jb + 8, :]
                rows.append(value)
        rows.append(jnp.zeros((8, 128), F32))
        turned = jnp.transpose(jnp.concatenate(rows, axis=0))
        packed_ref[g] = turned
        flat[g * NREG : (g + 1) * NREG, :] = turned
        south_edge[g] = flat[pl.ds(g * NREG, RX, stride=RY), :]
        north_edge[g] = flat[pl.ds(g * NREG + RY - 1, RX, stride=RY), :]
    flat[GROUPS * NREG : 16 * NREG, :] = jnp.zeros((2 * NREG, 128), F32)
    for c, r in enumerate((0, RY - 1, NREG - RY, NREG - 1)):
        corner_edge[c] = flat[pl.ds(r, 16, stride=NREG), :]

    plan = [
        (packed_ref.at[:, pl.ds(0, RY)], east_in, (-1, 0)),
        (packed_ref.at[:, pl.ds(NREG - RY, RY)], west_in, (1, 0)),
        (south_edge, north_in, (0, -1)),
        (north_edge, south_in, (0, 1)),
        (corner_edge.at[0], corner_in.at[3], (-1, -1)),
        (corner_edge.at[1], corner_in.at[2], (-1, 1)),
        (corner_edge.at[2], corner_in.at[1], (1, -1)),
        (corner_edge.at[3], corner_in.at[0], (1, 1)),
    ]
    copies = []
    for n, (src, dst, (dx, dy)) in enumerate(plan):
        copy = pltpu.make_async_remote_copy(
            src_ref=src,
            dst_ref=dst,
            send_sem=send_edge.at[n],
            recv_sem=recv_edge.at[n],
            device_id=device(dx, dy),
            device_id_type=MESH,
        )
        copy.start()
        copies.append(copy)
    for copy in copies:
        copy.wait()
    west_out[...] = west_in[...]
    east_out[...] = east_in[...]
    south_out[...] = south_in[...]
    north_out[...] = north_in[...]
    corner_out[...] = corner_in[...]


def analyse(obs, innovation, precision, column, count):
    shapes = [(GROUPS, RY, 128), (GROUPS, RY, 128), (GROUPS, RX, 128), (GROUPS, RX, 128), (4, 16, 128)]
    return pl.pallas_call(
        analyse_kernel,
        out_shape=tuple(jax.ShapeDtypeStruct(s, F32) for s in [(GROUPS, NREG, 128)] + shapes),
        in_specs=vmem_specs(5),
        out_specs=tuple(vmem_specs(6)),
        scratch_shapes=[
            pltpu.VMEM((9, ROWS, SLOTS), F32),
            pltpu.VMEM((1, 128), F32),
            pltpu.VMEM((1, 128), F32),
            pltpu.VMEM((NB, 1, 128), F32),
            pltpu.VMEM((NB, 1, 128), F32),
            pltpu.VMEM((1024, SLOTS), BF16),
            pltpu.VMEM((1024, SLOTS), BF16),
            pltpu.VMEM((1024, NREG), F32),
            pltpu.VMEM((M * M, 128), F32),
            pltpu.VMEM((M * M, 128), F32),
            pltpu.VMEM((16 * NREG, 128), F32),
            pltpu.VMEM((GROUPS, RX, 128), F32),
            pltpu.VMEM((GROUPS, RX, 128), F32),
            pltpu.VMEM((4, 16, 128), F32),
        ]
        + [pltpu.VMEM(s, F32) for s in shapes]
        + [
            pltpu.SemaphoreType.DMA((8,)),
            pltpu.SemaphoreType.DMA((8,)),
            pltpu.SemaphoreType.DMA((NB,)),
            pltpu.SemaphoreType.DMA((NB,)),
            pltpu.SemaphoreType.DMA((NB,)),
            pltpu.SemaphoreType.DMA((NB,)),
            pltpu.SemaphoreType.DMA((8,)),
            pltpu.SemaphoreType.DMA((8,)),
        ],
        compiler_params=pltpu.CompilerParams(collective_id=0, has_side_effects=True),
        name="analyse",
    )(obs, innovation, precision, column, count)


def apply_kernel(
    state_ref, packed_ref, west_ref, east_ref, south_ref, north_ref, corner_ref,
    out_ref,
    frame, line, weights, members, results, state, after, read_sem, write_sem,
):
    def reads(a):
        return pltpu.make_async_copy(state_ref.at[:, a], state.at[a], read_sem.at[a])

    def writes(a):
        return pltpu.make_async_copy(after.at[a], out_ref.at[:, a], write_sem.at[a])

    for a in range(CX):
        reads(a).start()

    gy = lax.axis_index("gy")
    bottom = gy == 0
    top = gy == NB - 1
    for g in range(GROUPS):
        frame[g, 0, 8:24, :] = west_ref[g]
        frame[g, RX + 1, 8:24, :] = east_ref[g]
        frame[g, 0, 7:8, :] = jnp.where(bottom, west_ref[g, 0:1], corner_ref[0, g : g + 1])
        frame[g, 0, 24:25, :] = jnp.where(top, west_ref[g, RY - 1 : RY], corner_ref[1, g : g + 1])
        frame[g, RX + 1, 7:8, :] = jnp.where(bottom, east_ref[g, 0:1], corner_ref[2, g : g + 1])
        frame[g, RX + 1, 24:25, :] = jnp.where(top, east_ref[g, RY - 1 : RY], corner_ref[3, g : g + 1])
        for p in range(RX):
            r = p * RY
            frame[g, p + 1, 8:24, :] = packed_ref[g, r : r + RY, :]
            frame[g, p + 1, 7:8, :] = jnp.where(
                bottom, packed_ref[g, r : r + 1, :], south_ref[g, p : p + 1]
            )
            frame[g, p + 1, 24:25, :] = jnp.where(
                top, packed_ref[g, r + RY - 1 : r + RY, :], north_ref[g, p : p + 1]
            )

    def strip(a, carry):
        reads(a).wait()
        p = lax.div(a, 2)
        odd = lax.rem(a, 2)
        for g in range(GROUPS):
            line[...] = 0.75 * frame[g, p + 1] + 0.25 * frame[g, p + 2 * odd]
            centre = 0.75 * line[8:24, :]
            weights[g * STRIDE : g * STRIDE + 16, :] = centre + 0.25 * line[7:23, :]
            weights[g * STRIDE + 16 : g * STRIDE + 32, :] = centre + 0.25 * line[9:25, :]
        for j in range(M):
            members[j * STRIDE : j * STRIDE + CY, :] = state[a, j].astype(F32)

        lane = lax.broadcasted_iota(jnp.int32, (16, 128), 1)
        low_side = lane >= M

        for y in range(CY):
            q, par = y // 2, y % 2
            block = members[pl.ds(y, M, stride=STRIDE), :].astype(BF16)
            block = jnp.concatenate([block, block], axis=0)
            value = weights[pl.ds(par * 16 + q, 16, stride=STRIDE), :]
            high = value.astype(BF16).astype(F32)
            low = value - high
            low40 = pltpu.roll(low, 128 - 40, 1)
            parts = [
                jnp.where(low_side, pltpu.roll(low, 40, 1), high),
                jnp.where(low_side, low, pltpu.roll(high, 128 - 40, 1)),
                jnp.where(low_side, low40, pltpu.roll(high, 128 - 80, 1)),
            ]
            left = jnp.concatenate([v.astype(BF16) for v in parts], axis=0)[:, : 2 * M]
            out = jnp.dot(left, block, preferred_element_type=F32)
            results[pl.ds(y, 14, stride=STRIDE), :] = out[0:14]
            results[pl.ds(14 * STRIDE + y, 14, stride=STRIDE), :] = out[16:30]
            results[pl.ds(28 * STRIDE + y, 12, stride=STRIDE), :] = out[32:44]
        for k in range(M):
            after[a, k] = results[k * STRIDE : k * STRIDE + CY, :].astype(BF16)
        writes(a).start()
        return carry

    lax.fori_loop(0, CX, strip, 0)
    for a in range(CX):
        writes(a).wait()


def apply(state, packed, west, east, south, north, corner):
    return pl.pallas_call(
        apply_kernel,
        out_shape=jax.ShapeDtypeStruct((M, CX, CY, 128), BF16),
        in_specs=[pl.BlockSpec(memory_space=pl.ANY)] + vmem_specs(6),
        out_specs=pl.BlockSpec(memory_space=pl.ANY),
        scratch_shapes=[
            pltpu.VMEM((GROUPS, RX + 2, 32, 128), F32),
            pltpu.VMEM((32, 128), F32),
            pltpu.VMEM((16 * STRIDE, 128), F32),
            pltpu.VMEM((M * STRIDE, 128), F32),
            pltpu.VMEM((M * STRIDE, 128), F32),
            pltpu.VMEM((CX, M, CY, 128), BF16),
            pltpu.VMEM((CX, M, CY, 128), BF16),
            pltpu.SemaphoreType.DMA((CX,)),
            pltpu.SemaphoreType.DMA((CX,)),
        ],
        name="apply",
    )(state, packed, west, east, south, north, corner)


def per_device(background, obs_perturb, innovation, obs_precision, obs_column, obs_count):
    parts = analyse(
        obs_perturb[0, 0], innovation[0], obs_precision[0], obs_column[0], obs_count
    )
    return apply(background, *parts)


def solution(mesh):
    return jax.shard_map(
        per_device,
        mesh=mesh,
        in_specs=(
            P(None, "gx", "gy", None),
            P("gx", "gy", None, None),
            P("gx", "gy", None),
            P("gx", "gy", None),
            P("gx", "gy", None),
            P("gx", "gy"),
        ),
        out_specs=P(None, "gx", "gy", None),
        check_vma=False,
    )
```

```python
import functools
import math

import jax
import jax.numpy as jnp
from jax import lax
from jax.experimental import pallas as pl
from jax.experimental.pallas import tpu as pltpu
from jax.sharding import PartitionSpec as P

F32 = jnp.float32
BF16 = jnp.bfloat16
MESH = pl.DeviceIdType.MESH
NB = 16
M = 40
SLOTS = 256
CX, CY = 16, 32
RX, RY = 8, 16
NREG = RX * RY
ROWS = 48
GROUPS = 14
STRIDE = 40
NEIGHBOURS = [(0, -1), (0, 1), (-1, 0), (1, 0), (-1, -1), (-1, 1), (1, -1), (1, 1)]


def vmem_specs(count):
    return [pl.BlockSpec(memory_space=pltpu.VMEM)] * count


BLOCKS = [(ib, jb) for ib in range(5) for jb in range(ib, 5)]


def split(value):
    high = value.astype(BF16)
    return high, (value - high.astype(F32)).astype(BF16)


def analyse_kernel(
    obs_ref, innovation_ref, precision_ref, column_ref, count_ref,
    packed_ref, west_out, east_out, south_out, north_out, corner_out,
    landed, part_a, part_b, slots_a, slots_b,
    table, gram, upper, inverse, flat,
    south_edge, north_edge, corner_edge,
    west_in, east_in, south_in, north_in, corner_in,
    send_near, recv_near, send_a, recv_a, send_b, recv_b, send_edge, recv_edge,
):
    gx = lax.axis_index("gx")
    gy = lax.axis_index("gy")

    def device(dx, dy):
        return (lax.rem(gx + dx + NB, NB), lax.rem(gy + dy + NB, NB))

    barrier = pltpu.get_barrier_semaphore()
    peers = [(0, d) for d in range(1, NB)] + [(d, 0) for d in range(1, NB)]
    peers += [(1, 1), (1, -1), (-1, 1), (-1, -1)]
    for dx, dy in peers:
        pl.semaphore_signal(barrier, inc=1, device_id=device(dx, dy), device_id_type=MESH)

    centered = obs_ref[...].astype(F32)
    centered = centered - jnp.sum(centered, axis=0, keepdims=True) * (1.0 / M)
    innovation = innovation_ref[...]
    slot = lax.broadcasted_iota(jnp.int32, (1, SLOTS), 1)
    weight = jnp.where(slot < count_ref[...], precision_ref[...], 0.0)
    column = column_ref[...]
    east = (gx * CX + lax.shift_right_logical(column, 5)).astype(F32) + 0.5
    north = (gy * CY + jnp.bitwise_and(column, 31)).astype(F32) + 0.5
    mine = landed.at[0]
    mine[0:M, :] = centered
    mine[M : M + 8, :] = jnp.concatenate(
        [innovation, weight, east, north, jnp.zeros((4, SLOTS), F32)], axis=0
    )
    numer = jnp.sum(weight * innovation * innovation, axis=1, keepdims=True)
    squares = jnp.sum(centered * centered, axis=0, keepdims=True)
    denom = jnp.sum(weight * squares, axis=1, keepdims=True) / (M - 1)
    lane = lax.broadcasted_iota(jnp.int32, (1, 128), 1)
    part = jnp.where(lane < 64, numer, denom)
    part_a[...] = part

    pl.semaphore_wait(barrier, len(peers))

    def spread(src, slots, send, recv, along_x):
        copies = []
        for d in range(1, NB):
            copy = pltpu.make_async_remote_copy(
                src_ref=src,
                dst_ref=slots.at[d],
                send_sem=send.at[d],
                recv_sem=recv.at[d],
                device_id=device(d, 0) if along_x else device(0, d),
                device_id_type=MESH,
            )
            copies.append(copy)
        return copies

    first = spread(part_a, slots_a, send_a, recv_a, False)
    for copy in first:
        copy.start()
    near = []
    for n, (dx, dy) in enumerate(NEIGHBOURS):
        copy = pltpu.make_async_remote_copy(
            src_ref=mine,
            dst_ref=landed.at[n + 1],
            send_sem=send_near.at[n],
            recv_sem=recv_near.at[n],
            device_id=device(dx, dy),
            device_id_type=MESH,
        )
        copy.start()
        near.append(copy)
    region = lax.broadcasted_iota(jnp.int32, (NREG, SLOTS), 0)
    centre_east = (gx * CX + 2 * lax.shift_right_logical(region, 4)).astype(F32) + 1.0
    centre_north = (gy * CY + 2 * jnp.bitwise_and(region, 15)).astype(F32) + 1.0
    gram[...] = jnp.zeros_like(gram)
    table[...] = jnp.zeros_like(table)

    def tile(t, carry):
        for n in range(8):

            @pl.when(t == n + 1)
            def arrive(copy=near[n]):
                copy.wait()

        @pl.when(t == 5)
        def relay():
            total = part_a[...]
            for copy in first:
                copy.wait()
            for d in range(1, NB):
                total = total + slots_a[d]
            part_b[...] = total
            for copy in spread(part_b, slots_b, send_b, recv_b, True):
                copy.start()

        obs = landed.at[t]
        east = obs[M + 2 : M + 3, :]
        north = obs[M + 3 : M + 4, :]
        weight = obs[M + 1 : M + 2, :]
        innovation = obs[M : M + 1, :]
        de = east - centre_east + 128.0
        de = jnp.where(de < 0.0, de + 256.0, de)
        de = jnp.where(de >= 256.0, de - 256.0, de) - 128.0
        dn = north - centre_north
        reach = jnp.maximum(1.0 - (de * de + dn * dn) * (1.0 / 256.0), 0.0)
        reach = reach * reach * weight
        reach_high, reach_low = split(reach)
        both = jnp.concatenate([reach_high, reach_low], axis=0)
        for b, (ib, jb) in enumerate(BLOCKS):
            right = obs[8 * jb : 8 * jb + 8, :]
            for ii in range(0, 8, 2):
                i = 8 * ib + ii
                rows = jnp.concatenate(
                    [obs[i : i + 1, :] * right, obs[i + 1 : i + 2, :] * right], axis=0
                )
                high, low = split(rows)
                at = b * 64 + ii * 8
                table[at : at + 16, :SLOTS] = high
                table[at : at + 16, SLOTS:] = low
        pull = jnp.concatenate([obs[0:M, :] * innovation, jnp.zeros((8, SLOTS), F32)], axis=0)
        high, low = split(pull)
        table[960:1008, :SLOTS] = high
        table[960:1008, SLOTS:] = low
        twice = jnp.concatenate([both, both], axis=1)
        for c in range(0, 1024, 256):
            out = lax.dot_general(
                table[c : c + 256, :], twice, (((1,), (1,)), ((), ())),
                preferred_element_type=F32,
            )
            gram[c : c + 256, :] += out[:, :128] + out[:, 128:]
        return carry

    lax.fori_loop(0, 9, tile, 0)

    lane = lax.broadcasted_iota(jnp.int32, (1, 128), 1)
    for copy in spread(part_b, slots_b, send_b, recv_b, True):
        copy.wait()
    both = part_b[...]
    for d in range(1, NB):
        both = both + slots_b[d]
    numer = jnp.sum(jnp.where(lane == 0, both, 0.0), axis=1, keepdims=True)
    denom = jnp.sum(jnp.where(lane == 64, both, 0.0), axis=1, keepdims=True)
    prior = jnp.broadcast_to((M - 1) / (numer / denom), (8, 128))
    sub = lax.broadcasted_iota(jnp.int32, (8, 128), 0)
    inverse[...] = jnp.zeros_like(inverse)
    offset = {pair: 64 * b for b, pair in enumerate(BLOCKS)}

    for ib in range(5):
        cols = list(range(ib, 5))
        state = []
        for t in range(8):
            row = []
            for jb in cols:
                at = offset[(ib, jb)] + 8 * t
                value = gram[at : at + 8, :]
                if jb == ib:
                    value = value + jnp.where(sub == t, prior, 0.0)
                row.append(value)
            row += [jnp.zeros((8, 128), F32)] * ib
            state.append(row)

        def eliminate(p, state):
            base = p * M
            line = [upper[pl.ds(pl.multiple_of(base + 8 * jb, 8), 8), :] for jb in cols]
            line += [inverse[pl.ds(pl.multiple_of(base + 8 * jb, 8), 8), :] for jb in range(ib)]
            new = []
            for t in range(8):
                factor = upper[pl.ds(base + 8 * ib + t, 1), :]
                factor = jnp.broadcast_to(factor, (8, 128))
                new.append([s - factor * v for s, v in zip(state[t], line)])
            return new

        if ib:
            state = lax.fori_loop(0, 8 * ib, eliminate, state, unroll=4)
        state = [
            row + [jnp.where(sub == t, 1.0, 0.0).astype(F32)] for t, row in enumerate(state)
        ]
        for t in range(8):
            scale = lax.rsqrt(jnp.broadcast_to(state[t][0][t : t + 1, :], (8, 128)))
            state[t] = [v * scale for v in state[t]]
            for s in range(t + 1, 8):
                factor = jnp.broadcast_to(state[t][0][s : s + 1, :], (8, 128))
                state[s] = [a - factor * v for a, v in zip(state[s], state[t])]
            p = 8 * ib + t
            for jb, value in zip(cols, state[t][: len(cols)]):
                upper[p * M + 8 * jb : p * M + 8 * jb + 8, :] = value
            for jb, value in enumerate(state[t][len(cols) :]):
                inverse[p * M + 8 * jb : p * M + 8 * jb + 8, :] = value

    pull = [gram[960 + 8 * jb : 968 + 8 * jb, :] for jb in range(5)]
    mean = [jnp.zeros((8, 128), F32)] * 5
    sums = []
    for k in range(M):
        rows = [inverse[k * M + 8 * jb : k * M + 8 * jb + 8, :] for jb in range(k // 8 + 1)]
        inner = rows[0] * pull[0]
        plain = rows[0]
        for jb in range(1, len(rows)):
            inner = inner + rows[jb] * pull[jb]
            plain = plain + rows[jb]
        inner = jnp.broadcast_to(jnp.sum(inner, axis=0, keepdims=True), (8, 128))
        sums.append(jnp.broadcast_to(jnp.sum(plain, axis=0, keepdims=True), (8, 128)))
        for jb in range(len(rows)):
            mean[jb] = mean[jb] + rows[jb] * inner
    mean_sum = mean[0] + mean[1] + mean[2] + mean[3] + mean[4]
    mean_sum = jnp.broadcast_to(jnp.sum(mean_sum, axis=0, keepdims=True), (8, 128))
    root = math.sqrt(M - 1)
    for g in range(GROUPS):
        rows = []
        for part in range(3):
            k = part * GROUPS + g
            if k >= M:
                rows += [jnp.zeros((8, 128), F32)] * 5
                continue
            shift = (1.0 - mean_sum - root * sums[k]) * (1.0 / M)
            for jb in range(5):
                value = mean[jb] + shift
                if jb <= k // 8:
                    value = value + root * inverse[k * M + 8 * jb : k * M + 8 * jb + 8, :]
                rows.append(value)
        rows.append(jnp.zeros((8, 128), F32))
        turned = jnp.transpose(jnp.concatenate(rows, axis=0))
        packed_ref[g] = turned.reshape(RX, RY, 128)
        flat[g * NREG : (g + 1) * NREG, :] = turned
        south_edge[g] = flat[pl.ds(g * NREG, RX, stride=RY), :]
        north_edge[g] = flat[pl.ds(g * NREG + RY - 1, RX, stride=RY), :]
    flat[GROUPS * NREG : 16 * NREG, :] = jnp.zeros((2 * NREG, 128), F32)
    for c, r in enumerate((0, RY - 1, NREG - RY, NREG - 1)):
        corner_edge[c] = flat[pl.ds(r, 16, stride=NREG), :]

    plan = [
        (packed_ref.at[:, 0], east_in, (-1, 0)),
        (packed_ref.at[:, RX - 1], west_in, (1, 0)),
        (south_edge, north_in, (0, -1)),
        (north_edge, south_in, (0, 1)),
        (corner_edge.at[0], corner_in.at[3], (-1, -1)),
        (corner_edge.at[1], corner_in.at[2], (-1, 1)),
        (corner_edge.at[2], corner_in.at[1], (1, -1)),
        (corner_edge.at[3], corner_in.at[0], (1, 1)),
    ]
    copies = []
    for n, (src, dst, (dx, dy)) in enumerate(plan):
        copy = pltpu.make_async_remote_copy(
            src_ref=src,
            dst_ref=dst,
            send_sem=send_edge.at[n],
            recv_sem=recv_edge.at[n],
            device_id=device(dx, dy),
            device_id_type=MESH,
        )
        copy.start()
        copies.append(copy)
    for copy in copies:
        copy.wait()
    west_out[...] = west_in[...]
    east_out[...] = east_in[...]
    south_out[...] = south_in[...]
    north_out[...] = north_in[...]
    corner_out[...] = corner_in[...]


def analyse(obs, innovation, precision, column, count):
    shapes = [(GROUPS, RY, 128), (GROUPS, RY, 128), (GROUPS, RX, 128), (GROUPS, RX, 128), (4, 16, 128)]
    return pl.pallas_call(
        analyse_kernel,
        out_shape=tuple(jax.ShapeDtypeStruct(s, F32) for s in [(GROUPS, RX, RY, 128)] + shapes),
        in_specs=vmem_specs(5),
        out_specs=tuple(vmem_specs(6)),
        scratch_shapes=[
            pltpu.VMEM((9, ROWS, SLOTS), F32),
            pltpu.VMEM((1, 128), F32),
            pltpu.VMEM((1, 128), F32),
            pltpu.VMEM((NB, 1, 128), F32),
            pltpu.VMEM((NB, 1, 128), F32),
            pltpu.VMEM((1024, 2 * SLOTS), BF16),
            pltpu.VMEM((1024, NREG), F32),
            pltpu.VMEM((M * M, 128), F32),
            pltpu.VMEM((M * M, 128), F32),
            pltpu.VMEM((16 * NREG, 128), F32),
            pltpu.VMEM((GROUPS, RX, 128), F32),
            pltpu.VMEM((GROUPS, RX, 128), F32),
            pltpu.VMEM((4, 16, 128), F32),
        ]
        + [pltpu.VMEM(s, F32) for s in shapes]
        + [
            pltpu.SemaphoreType.DMA((8,)),
            pltpu.SemaphoreType.DMA((8,)),
            pltpu.SemaphoreType.DMA((NB,)),
            pltpu.SemaphoreType.DMA((NB,)),
            pltpu.SemaphoreType.DMA((NB,)),
            pltpu.SemaphoreType.DMA((NB,)),
            pltpu.SemaphoreType.DMA((8,)),
            pltpu.SemaphoreType.DMA((8,)),
        ],
        compiler_params=pltpu.CompilerParams(collective_id=0, has_side_effects=True),
        name="analyse",
    )(obs, innovation, precision, column, count)


def apply_kernel(
    state_ref, packed_ref, west_ref, east_ref, south_ref, north_ref, corner_ref,
    out_ref,
    frame, south, north, corner, state, after,
    weights_0, weights_1, members_0, members_1, results_0, results_1,
    frame_sem, read_sem, write_sem,
):
    weights = (weights_0, weights_1)
    members = (members_0, members_1)
    results = (results_0, results_1)

    def reads(a):
        return pltpu.make_async_copy(state_ref.at[:, a], state.at[a], read_sem.at[a])

    def writes(a):
        return pltpu.make_async_copy(after.at[a], out_ref.at[:, a], write_sem.at[a])

    reads(0).start()
    loads = [
        (packed_ref, frame.at[:, pl.ds(1, RX), pl.ds(8, RY)]),
        (west_ref, frame.at[:, 0, pl.ds(8, RY)]),
        (east_ref, frame.at[:, RX + 1, pl.ds(8, RY)]),
        (south_ref, south),
        (north_ref, north),
        (corner_ref, corner),
    ]
    loads = [
        pltpu.make_async_copy(src, dst, frame_sem.at[n]) for n, (src, dst) in enumerate(loads)
    ]
    for copy in loads:
        copy.start()
    for a in range(1, CX):
        reads(a).start()

    def take(j, a, half):
        members[half][j * STRIDE : j * STRIDE + CY, :] = state[a, j].astype(F32)

    def blend(g, p, half):
        def east(start):
            near = frame[g, p + 1, start : start + 16, :]
            far = frame[g, p + 2 * half, start : start + 16, :]
            return 0.75 * near + 0.25 * far

        centre = 0.75 * east(8)
        weights[half][g * STRIDE : g * STRIDE + 16, :] = centre + 0.25 * east(7)
        weights[half][g * STRIDE + 16 : g * STRIDE + 32, :] = centre + 0.25 * east(9)

    def give(k, a, half):
        after[a, k] = results[half][k * STRIDE : k * STRIDE + CY, :].astype(BF16)

    lane = lax.broadcasted_iota(jnp.int32, (16, 128), 1)
    low_side = lane >= M

    def column(y, half):
        q, par = y // 2, y % 2
        block = members[half][pl.ds(y, M, stride=STRIDE), :].astype(BF16)
        block = jnp.concatenate([block, block], axis=0)
        value = weights[half][pl.ds(par * 16 + q, 16, stride=STRIDE), :]
        high = value.astype(BF16).astype(F32)
        low = value - high
        parts = [
            jnp.where(low_side, pltpu.roll(low, 40, 1), high),
            jnp.where(low_side, low, pltpu.roll(high, 128 - 40, 1)),
            jnp.where(low_side, pltpu.roll(low, 128 - 40, 1), pltpu.roll(high, 128 - 80, 1)),
        ]
        left = jnp.concatenate([v.astype(BF16) for v in parts], axis=0)[:, : 2 * M]
        out = jnp.dot(left, block, preferred_element_type=F32)
        result = results[half]
        result[pl.ds(y, 14, stride=STRIDE), :] = out[0:14]
        result[pl.ds(14 * STRIDE + y, 14, stride=STRIDE), :] = out[16:30]
        result[pl.ds(28 * STRIDE + y, 12, stride=STRIDE), :] = out[32:44]

    reads(0).wait()
    for j in range(M):
        take(j, 0, 0)
    for copy in loads:
        copy.wait()
    gy = lax.axis_index("gy")
    bottom = gy == 0
    top = gy == NB - 1
    for g in range(GROUPS):
        for p in range(RX + 2):
            if p == 0:
                below, above = corner[0, g : g + 1], corner[1, g : g + 1]
            elif p == RX + 1:
                below, above = corner[2, g : g + 1], corner[3, g : g + 1]
            else:
                below, above = south[g, p - 1 : p], north[g, p - 1 : p]
            frame[g, p, 7:8, :] = jnp.where(bottom, frame[g, p, 8:9, :], below)
            frame[g, p, 24:25, :] = jnp.where(top, frame[g, p, 23:24, :], above)
    for g in range(GROUPS):
        blend(g, 0, 0)

    def pair(i, carry):
        for half in range(2):
            a = 2 * i + half
            later = jnp.minimum(a + 1, CX - 1)
            before = jnp.maximum(a - 1, 0)

            @pl.when(a + 1 < CX)
            def arrive():
                reads(later).wait()

            jobs = [functools.partial(give, k, before, 1 - half) for k in range(M)]
            jobs += [functools.partial(blend, g, lax.div(later, 2), 1 - half) for g in range(GROUPS)]
            jobs += [functools.partial(take, j, later, 1 - half) for j in range(M)]
            done = 0
            for y in range(CY):
                column(y, half)
                until = (y + 1) * len(jobs) // CY
                for job in jobs[done:until]:
                    job()
                done = until

            @pl.when(a > 0)
            def leave():
                writes(before).start()

        return carry

    lax.fori_loop(0, CX // 2, pair, 0)
    for k in range(M):
        give(k, CX - 1, 1)
    writes(CX - 1).start()
    for a in range(CX):
        writes(a).wait()


def apply(state, packed, west, east, south, north, corner):
    return pl.pallas_call(
        apply_kernel,
        out_shape=jax.ShapeDtypeStruct((M, CX, CY, 128), BF16),
        in_specs=[pl.BlockSpec(memory_space=pl.ANY)] * 7,
        out_specs=pl.BlockSpec(memory_space=pl.ANY),
        scratch_shapes=[
            pltpu.VMEM((GROUPS, RX + 2, 32, 128), F32),
            pltpu.VMEM((GROUPS, RX, 128), F32),
            pltpu.VMEM((GROUPS, RX, 128), F32),
            pltpu.VMEM((4, 16, 128), F32),
            pltpu.VMEM((CX, M, CY, 128), BF16),
            pltpu.VMEM((CX, M, CY, 128), BF16),
            pltpu.VMEM((16 * STRIDE, 128), F32),
            pltpu.VMEM((16 * STRIDE, 128), F32),
            pltpu.VMEM((M * STRIDE, 128), F32),
            pltpu.VMEM((M * STRIDE, 128), F32),
            pltpu.VMEM((M * STRIDE, 128), F32),
            pltpu.VMEM((M * STRIDE, 128), F32),
            pltpu.SemaphoreType.DMA((6,)),
            pltpu.SemaphoreType.DMA((CX,)),
            pltpu.SemaphoreType.DMA((CX,)),
        ],
        name="apply",
    )(state, packed, west, east, south, north, corner)


def per_device(background, obs_perturb, innovation, obs_precision, obs_column, obs_count):
    parts = analyse(
        obs_perturb[0, 0], innovation[0], obs_precision[0], obs_column[0], obs_count
    )
    return apply(background, *parts)


def solution(mesh):
    return jax.shard_map(
        per_device,
        mesh=mesh,
        in_specs=(
            P(None, "gx", "gy", None),
            P("gx", "gy", None, None),
            P("gx", "gy", None),
            P("gx", "gy", None),
            P("gx", "gy", None),
            P("gx", "gy"),
        ),
        out_specs=P(None, "gx", "gy", None),
        check_vma=False,
    )
```

```python
import functools
import math

import jax
import jax.numpy as jnp
from jax import lax
from jax.experimental import pallas as pl
from jax.experimental.pallas import tpu as pltpu
from jax.sharding import PartitionSpec as P

F32 = jnp.float32
BF16 = jnp.bfloat16
MESH = pl.DeviceIdType.MESH
NB = 16
M = 40
SLOTS = 256
CX, CY = 16, 32
RX, RY = 8, 16
NREG = RX * RY
ROWS = 48
GROUPS = 14
AHEAD = 4
STRIDE = 40
NEIGHBOURS = [(0, -1), (0, 1), (-1, 0), (1, 0), (-1, -1), (-1, 1), (1, -1), (1, 1)]


def vmem_specs(count):
    return [pl.BlockSpec(memory_space=pltpu.VMEM)] * count


BLOCKS = [(ib, jb) for ib in range(5) for jb in range(ib, 5)]


def split(value):
    high = value.astype(BF16)
    return high, (value - high.astype(F32)).astype(BF16)


def analyse_kernel(
    obs_ref, innovation_ref, precision_ref, column_ref, count_ref,
    packed_out, west_in, east_in, south_in, north_in, corner_in,
    landed, part_a, part_b, slots_a, slots_b,
    table, gram, upper, inverse, flat,
    packed_ref, south_edge, north_edge, corner_edge,
    send_near, recv_near, send_a, recv_a, send_b, recv_b, send_edge, recv_edge, packed_sem,
):
    gx = lax.axis_index("gx")
    gy = lax.axis_index("gy")

    def device(dx, dy):
        return (lax.rem(gx + dx + NB, NB), lax.rem(gy + dy + NB, NB))

    barrier = pltpu.get_barrier_semaphore()
    peers = [(0, d) for d in range(1, NB)] + [(d, 0) for d in range(1, NB)]
    peers += [(1, 1), (1, -1), (-1, 1), (-1, -1)]
    for dx, dy in peers:
        pl.semaphore_signal(barrier, inc=1, device_id=device(dx, dy), device_id_type=MESH)

    centered = obs_ref[...].astype(F32)
    centered = centered - jnp.sum(centered, axis=0, keepdims=True) * (1.0 / M)
    innovation = innovation_ref[...]
    slot = lax.broadcasted_iota(jnp.int32, (1, SLOTS), 1)
    weight = jnp.where(slot < count_ref[...], precision_ref[...], 0.0)
    column = column_ref[...]
    east = (gx * CX + lax.shift_right_logical(column, 5)).astype(F32) + 0.5
    north = (gy * CY + jnp.bitwise_and(column, 31)).astype(F32) + 0.5
    mine = landed.at[0]
    mine[0:M, :] = centered
    mine[M : M + 8, :] = jnp.concatenate(
        [innovation, weight, east, north, jnp.zeros((4, SLOTS), F32)], axis=0
    )
    numer = jnp.sum(weight * innovation * innovation, axis=1, keepdims=True)
    squares = jnp.sum(centered * centered, axis=0, keepdims=True)
    denom = jnp.sum(weight * squares, axis=1, keepdims=True) / (M - 1)
    lane = lax.broadcasted_iota(jnp.int32, (1, 128), 1)
    part = jnp.where(lane < 64, numer, denom)
    part_a[...] = part

    pl.semaphore_wait(barrier, len(peers))

    def spread(src, slots, send, recv, along_x):
        copies = []
        for d in range(1, NB):
            copy = pltpu.make_async_remote_copy(
                src_ref=src,
                dst_ref=slots.at[d],
                send_sem=send.at[d],
                recv_sem=recv.at[d],
                device_id=device(d, 0) if along_x else device(0, d),
                device_id_type=MESH,
            )
            copies.append(copy)
        return copies

    first = spread(part_a, slots_a, send_a, recv_a, False)
    for copy in first:
        copy.start()
    near = []
    for n, (dx, dy) in enumerate(NEIGHBOURS):
        copy = pltpu.make_async_remote_copy(
            src_ref=mine,
            dst_ref=landed.at[n + 1],
            send_sem=send_near.at[n],
            recv_sem=recv_near.at[n],
            device_id=device(dx, dy),
            device_id_type=MESH,
        )
        copy.start()
        near.append(copy)
    region = lax.broadcasted_iota(jnp.int32, (NREG, SLOTS), 0)
    centre_east = (gx * CX + 2 * lax.shift_right_logical(region, 4)).astype(F32) + 1.0
    centre_north = (gy * CY + 2 * jnp.bitwise_and(region, 15)).astype(F32) + 1.0
    gram[...] = jnp.zeros_like(gram)
    table[...] = jnp.zeros_like(table)

    def tile(t, carry):
        for n in range(8):

            @pl.when(t == n + 1)
            def arrive(copy=near[n]):
                copy.wait()

        @pl.when(t == 5)
        def relay():
            total = part_a[...]
            for copy in first:
                copy.wait()
            for d in range(1, NB):
                total = total + slots_a[d]
            part_b[...] = total
            for copy in spread(part_b, slots_b, send_b, recv_b, True):
                copy.start()

        obs = landed.at[t]
        east = obs[M + 2 : M + 3, :]
        north = obs[M + 3 : M + 4, :]
        weight = obs[M + 1 : M + 2, :]
        innovation = obs[M : M + 1, :]
        de = east - centre_east + 128.0
        de = jnp.where(de < 0.0, de + 256.0, de)
        de = jnp.where(de >= 256.0, de - 256.0, de) - 128.0
        dn = north - centre_north
        reach = jnp.maximum(1.0 - (de * de + dn * dn) * (1.0 / 256.0), 0.0)
        reach = reach * reach * weight
        reach_high, reach_low = split(reach)
        both = jnp.concatenate([reach_high, reach_low], axis=0)
        for b, (ib, jb) in enumerate(BLOCKS):
            right = obs[8 * jb : 8 * jb + 8, :]
            for ii in range(0, 8, 2):
                i = 8 * ib + ii
                rows = jnp.concatenate(
                    [obs[i : i + 1, :] * right, obs[i + 1 : i + 2, :] * right], axis=0
                )
                high, low = split(rows)
                at = b * 64 + ii * 8
                table[at : at + 16, :SLOTS] = high
                table[at : at + 16, SLOTS:] = low
        pull = jnp.concatenate([obs[0:M, :] * innovation, jnp.zeros((8, SLOTS), F32)], axis=0)
        high, low = split(pull)
        table[960:1008, :SLOTS] = high
        table[960:1008, SLOTS:] = low
        twice = jnp.concatenate([both, both], axis=1)
        for c in range(0, 1024, 256):
            out = lax.dot_general(
                table[c : c + 256, :], twice, (((1,), (1,)), ((), ())),
                preferred_element_type=F32,
            )
            gram[c : c + 256, :] += out[:, :128] + out[:, 128:]
        return carry

    lax.fori_loop(0, 9, tile, 0)

    lane = lax.broadcasted_iota(jnp.int32, (1, 128), 1)
    for copy in spread(part_b, slots_b, send_b, recv_b, True):
        copy.wait()
    both = part_b[...]
    for d in range(1, NB):
        both = both + slots_b[d]
    numer = jnp.sum(jnp.where(lane == 0, both, 0.0), axis=1, keepdims=True)
    denom = jnp.sum(jnp.where(lane == 64, both, 0.0), axis=1, keepdims=True)
    prior = jnp.broadcast_to((M - 1) / (numer / denom), (8, 128))
    sub = lax.broadcasted_iota(jnp.int32, (8, 128), 0)
    inverse[...] = jnp.zeros_like(inverse)
    offset = {pair: 64 * b for b, pair in enumerate(BLOCKS)}

    for ib in range(5):
        cols = list(range(ib, 5))
        state = []
        for t in range(8):
            row = []
            for jb in cols:
                at = offset[(ib, jb)] + 8 * t
                value = gram[at : at + 8, :]
                if jb == ib:
                    value = value + jnp.where(sub == t, prior, 0.0)
                row.append(value)
            row += [jnp.zeros((8, 128), F32)] * ib
            state.append(row)

        def eliminate(p, state):
            base = p * M
            line = [upper[pl.ds(pl.multiple_of(base + 8 * jb, 8), 8), :] for jb in cols]
            line += [inverse[pl.ds(pl.multiple_of(base + 8 * jb, 8), 8), :] for jb in range(ib)]
            new = []
            for t in range(8):
                factor = upper[pl.ds(base + 8 * ib + t, 1), :]
                factor = jnp.broadcast_to(factor, (8, 128))
                new.append([s - factor * v for s, v in zip(state[t], line)])
            return new

        if ib:
            state = lax.fori_loop(0, 8 * ib, eliminate, state, unroll=4)
        state = [
            row + [jnp.where(sub == t, 1.0, 0.0).astype(F32)] for t, row in enumerate(state)
        ]
        for t in range(8):
            scale = lax.rsqrt(jnp.broadcast_to(state[t][0][t : t + 1, :], (8, 128)))
            state[t] = [v * scale for v in state[t]]
            for s in range(t + 1, 8):
                factor = jnp.broadcast_to(state[t][0][s : s + 1, :], (8, 128))
                state[s] = [a - factor * v for a, v in zip(state[s], state[t])]
            p = 8 * ib + t
            for jb, value in zip(cols, state[t][: len(cols)]):
                upper[p * M + 8 * jb : p * M + 8 * jb + 8, :] = value
            for jb, value in enumerate(state[t][len(cols) :]):
                inverse[p * M + 8 * jb : p * M + 8 * jb + 8, :] = value

    pull = [gram[960 + 8 * jb : 968 + 8 * jb, :] for jb in range(5)]
    mean = [jnp.zeros((8, 128), F32)] * 5
    sums = []
    for k in range(M):
        rows = [inverse[k * M + 8 * jb : k * M + 8 * jb + 8, :] for jb in range(k // 8 + 1)]
        inner = rows[0] * pull[0]
        plain = rows[0]
        for jb in range(1, len(rows)):
            inner = inner + rows[jb] * pull[jb]
            plain = plain + rows[jb]
        inner = jnp.broadcast_to(jnp.sum(inner, axis=0, keepdims=True), (8, 128))
        sums.append(jnp.broadcast_to(jnp.sum(plain, axis=0, keepdims=True), (8, 128)))
        for jb in range(len(rows)):
            mean[jb] = mean[jb] + rows[jb] * inner
    mean_sum = mean[0] + mean[1] + mean[2] + mean[3] + mean[4]
    mean_sum = jnp.broadcast_to(jnp.sum(mean_sum, axis=0, keepdims=True), (8, 128))
    root = math.sqrt(M - 1)
    for g in range(GROUPS):
        rows = []
        for part in range(3):
            k = part * GROUPS + g
            if k >= M:
                rows += [jnp.zeros((8, 128), F32)] * 5
                continue
            shift = (1.0 - mean_sum - root * sums[k]) * (1.0 / M)
            for jb in range(5):
                value = mean[jb] + shift
                if jb <= k // 8:
                    value = value + root * inverse[k * M + 8 * jb : k * M + 8 * jb + 8, :]
                rows.append(value)
        rows.append(jnp.zeros((8, 128), F32))
        turned = jnp.transpose(jnp.concatenate(rows, axis=0))
        packed_ref[g] = turned.reshape(RX, RY, 128)
        flat[g * NREG : (g + 1) * NREG, :] = turned
        south_edge[g] = flat[pl.ds(g * NREG, RX, stride=RY), :]
        north_edge[g] = flat[pl.ds(g * NREG + RY - 1, RX, stride=RY), :]
    flat[GROUPS * NREG : 16 * NREG, :] = jnp.zeros((2 * NREG, 128), F32)
    for c, r in enumerate((0, RY - 1, NREG - RY, NREG - 1)):
        corner_edge[c] = flat[pl.ds(r, 16, stride=NREG), :]

    plan = [
        (packed_ref.at[:, 0], east_in, (-1, 0)),
        (packed_ref.at[:, RX - 1], west_in, (1, 0)),
        (south_edge, north_in, (0, -1)),
        (north_edge, south_in, (0, 1)),
        (corner_edge.at[0], corner_in.at[3], (-1, -1)),
        (corner_edge.at[1], corner_in.at[2], (-1, 1)),
        (corner_edge.at[2], corner_in.at[1], (1, -1)),
        (corner_edge.at[3], corner_in.at[0], (1, 1)),
    ]
    copies = []
    for n, (src, dst, (dx, dy)) in enumerate(plan):
        copy = pltpu.make_async_remote_copy(
            src_ref=src,
            dst_ref=dst,
            send_sem=send_edge.at[n],
            recv_sem=recv_edge.at[n],
            device_id=device(dx, dy),
            device_id_type=MESH,
        )
        copy.start()
        copies.append(copy)
    leave = pltpu.make_async_copy(packed_ref, packed_out, packed_sem)
    leave.start()
    for copy in copies:
        copy.wait()
    leave.wait()


def analyse(obs, innovation, precision, column, count):
    shapes = [(GROUPS, RY, 128), (GROUPS, RY, 128), (GROUPS, RX, 128), (GROUPS, RX, 128), (4, 16, 128)]
    return pl.pallas_call(
        analyse_kernel,
        out_shape=tuple(jax.ShapeDtypeStruct(s, F32) for s in [(GROUPS, RX, RY, 128)] + shapes),
        in_specs=vmem_specs(5),
        out_specs=(pl.BlockSpec(memory_space=pl.ANY),) * 6,
        scratch_shapes=[
            pltpu.VMEM((9, ROWS, SLOTS), F32),
            pltpu.VMEM((1, 128), F32),
            pltpu.VMEM((1, 128), F32),
            pltpu.VMEM((NB, 1, 128), F32),
            pltpu.VMEM((NB, 1, 128), F32),
            pltpu.VMEM((1024, 2 * SLOTS), BF16),
            pltpu.VMEM((1024, NREG), F32),
            pltpu.VMEM((M * M, 128), F32),
            pltpu.VMEM((M * M, 128), F32),
            pltpu.VMEM((16 * NREG, 128), F32),
            pltpu.VMEM((GROUPS, RX, RY, 128), F32),
            pltpu.VMEM((GROUPS, RX, 128), F32),
            pltpu.VMEM((GROUPS, RX, 128), F32),
            pltpu.VMEM((4, 16, 128), F32),
            pltpu.SemaphoreType.DMA((8,)),
            pltpu.SemaphoreType.DMA((8,)),
            pltpu.SemaphoreType.DMA((NB,)),
            pltpu.SemaphoreType.DMA((NB,)),
            pltpu.SemaphoreType.DMA((NB,)),
            pltpu.SemaphoreType.DMA((NB,)),
            pltpu.SemaphoreType.DMA((8,)),
            pltpu.SemaphoreType.DMA((8,)),
            pltpu.SemaphoreType.DMA,
        ],
        compiler_params=pltpu.CompilerParams(collective_id=0, has_side_effects=True),
        name="analyse",
    )(obs, innovation, precision, column, count)


def apply_kernel(
    state_ref, packed_ref, west_ref, east_ref, south_ref, north_ref, corner_ref,
    out_ref,
    frame, south, north, corner, state, after,
    weights_0, weights_1, members_0, members_1, results_0, results_1,
    frame_sem, read_sem, write_sem,
):
    weights = (weights_0, weights_1)
    members = (members_0, members_1)
    results = (results_0, results_1)

    def reads(a):
        return pltpu.make_async_copy(state_ref.at[:, a], state.at[a], read_sem.at[a])

    def writes(a):
        return pltpu.make_async_copy(after.at[a], out_ref.at[:, a], write_sem.at[a])

    reads(0).start()
    loads = [
        (packed_ref, frame.at[:, pl.ds(1, RX), pl.ds(8, RY)]),
        (west_ref, frame.at[:, 0, pl.ds(8, RY)]),
        (east_ref, frame.at[:, RX + 1, pl.ds(8, RY)]),
        (south_ref, south),
        (north_ref, north),
        (corner_ref, corner),
    ]
    loads = [
        pltpu.make_async_copy(src, dst, frame_sem.at[n]) for n, (src, dst) in enumerate(loads)
    ]
    for copy in loads:
        copy.start()
    for a in range(1, AHEAD):
        reads(a).start()

    def take(j, a, half):
        members[half][j * STRIDE : j * STRIDE + CY, :] = state[a, j].astype(F32)

    def blend(g, p, half):
        def east(start):
            near = frame[g, p + 1, start : start + 16, :]
            far = frame[g, p + 2 * half, start : start + 16, :]
            return 0.75 * near + 0.25 * far

        centre = 0.75 * east(8)
        weights[half][g * STRIDE : g * STRIDE + 16, :] = centre + 0.25 * east(7)
        weights[half][g * STRIDE + 16 : g * STRIDE + 32, :] = centre + 0.25 * east(9)

    def give(k, a, half):
        after[a, k] = results[half][k * STRIDE : k * STRIDE + CY, :].astype(BF16)

    lane = lax.broadcasted_iota(jnp.int32, (16, 128), 1)
    low_side = lane >= M

    def column(y, half):
        q, par = y // 2, y % 2
        block = members[half][pl.ds(y, M, stride=STRIDE), :].astype(BF16)
        block = jnp.concatenate([block, block], axis=0)
        value = weights[half][pl.ds(par * 16 + q, 16, stride=STRIDE), :]
        high = value.astype(BF16)
        low = (value - high.astype(F32)).astype(BF16)
        left = jnp.concatenate([
            jnp.where(low_side, pltpu.roll(low, 40, 1), high),
            jnp.where(low_side, low, pltpu.roll(high, 128 - 40, 1)),
            jnp.where(low_side, pltpu.roll(low, 128 - 40, 1), pltpu.roll(high, 128 - 80, 1)),
        ], axis=0)[:, : 2 * M]
        out = jnp.dot(left, block, preferred_element_type=F32)
        result = results[half]
        result[pl.ds(y, 14, stride=STRIDE), :] = out[0:14]
        result[pl.ds(14 * STRIDE + y, 14, stride=STRIDE), :] = out[16:30]
        result[pl.ds(28 * STRIDE + y, 12, stride=STRIDE), :] = out[32:44]

    reads(0).wait()
    for j in range(M):
        take(j, 0, 0)
    for copy in loads:
        copy.wait()
    gy = lax.axis_index("gy")
    bottom = gy == 0
    top = gy == NB - 1
    for g in range(GROUPS):
        for p in range(RX + 2):
            if p == 0:
                below, above = corner[0, g : g + 1], corner[1, g : g + 1]
            elif p == RX + 1:
                below, above = corner[2, g : g + 1], corner[3, g : g + 1]
            else:
                below, above = south[g, p - 1 : p], north[g, p - 1 : p]
            frame[g, p, 7:8, :] = jnp.where(bottom, frame[g, p, 8:9, :], below)
            frame[g, p, 24:25, :] = jnp.where(top, frame[g, p, 23:24, :], above)
    for g in range(GROUPS):
        blend(g, 0, 0)

    def pair(i, carry):
        for half in range(2):
            a = 2 * i + half
            later = jnp.minimum(a + 1, CX - 1)
            before = jnp.maximum(a - 1, 0)

            @pl.when(a + 1 < CX)
            def arrive():
                reads(later).wait()

            @pl.when(a + AHEAD < CX)
            def ahead():
                reads(jnp.minimum(a + AHEAD, CX - 1)).start()

            jobs = [functools.partial(give, k, before, 1 - half) for k in range(M)]
            jobs += [functools.partial(blend, g, lax.div(later, 2), 1 - half) for g in range(GROUPS)]
            jobs += [functools.partial(take, j, later, 1 - half) for j in range(M)]
            done = 0
            for y in range(CY):
                column(y, half)
                until = (y + 1) * len(jobs) // CY
                for job in jobs[done:until]:
                    job()
                done = until

            @pl.when(a > 0)
            def leave():
                writes(before).start()

        return carry

    lax.fori_loop(0, CX // 2, pair, 0)
    for k in range(M):
        give(k, CX - 1, 1)
    writes(CX - 1).start()
    for a in range(CX):
        writes(a).wait()


def apply(state, packed, west, east, south, north, corner):
    return pl.pallas_call(
        apply_kernel,
        out_shape=jax.ShapeDtypeStruct((M, CX, CY, 128), BF16),
        in_specs=[pl.BlockSpec(memory_space=pl.ANY)] * 7,
        out_specs=pl.BlockSpec(memory_space=pl.ANY),
        scratch_shapes=[
            pltpu.VMEM((GROUPS, RX + 2, 32, 128), F32),
            pltpu.VMEM((GROUPS, RX, 128), F32),
            pltpu.VMEM((GROUPS, RX, 128), F32),
            pltpu.VMEM((4, 16, 128), F32),
            pltpu.VMEM((CX, M, CY, 128), BF16),
            pltpu.VMEM((CX, M, CY, 128), BF16),
            pltpu.VMEM((16 * STRIDE, 128), F32),
            pltpu.VMEM((16 * STRIDE, 128), F32),
            pltpu.VMEM((M * STRIDE, 128), F32),
            pltpu.VMEM((M * STRIDE, 128), F32),
            pltpu.VMEM((M * STRIDE, 128), F32),
            pltpu.VMEM((M * STRIDE, 128), F32),
            pltpu.SemaphoreType.DMA((6,)),
            pltpu.SemaphoreType.DMA((CX,)),
            pltpu.SemaphoreType.DMA((CX,)),
        ],
        name="apply",
    )(state, packed, west, east, south, north, corner)


def per_device(background, obs_perturb, innovation, obs_precision, obs_column, obs_count):
    parts = analyse(
        obs_perturb[0, 0], innovation[0], obs_precision[0], obs_column[0], obs_count
    )
    return apply(background, *parts)


def solution(mesh):
    return jax.shard_map(
        per_device,
        mesh=mesh,
        in_specs=(
            P(None, "gx", "gy", None),
            P("gx", "gy", None, None),
            P("gx", "gy", None),
            P("gx", "gy", None),
            P("gx", "gy", None),
            P("gx", "gy"),
        ),
        out_specs=P(None, "gx", "gy", None),
        check_vma=False,
    )
```

```python
import functools
import math

import jax
import jax.numpy as jnp
from jax import lax
from jax.experimental import pallas as pl
from jax.experimental.pallas import tpu as pltpu
from jax.sharding import PartitionSpec as P

F32 = jnp.float32
BF16 = jnp.bfloat16
MESH = pl.DeviceIdType.MESH
NB = 16
M = 40
SLOTS = 256
CX, CY = 16, 32
RX, RY = 8, 16
NREG = RX * RY
ROWS = 48
GROUPS = 14
AHEAD = 4
STRIDE = 40
NEIGHBOURS = [(0, -1), (0, 1), (-1, 0), (1, 0), (-1, -1), (-1, 1), (1, -1), (1, 1)]


def vmem_specs(count):
    return [pl.BlockSpec(memory_space=pltpu.VMEM)] * count


BLOCKS = [(ib, jb) for ib in range(5) for jb in range(ib, 5)]


def split(value):
    high = value.astype(BF16)
    return high, (value - high.astype(F32)).astype(BF16)


def analyse_kernel(
    obs_in, innovation_in, precision_in, column_in, count_ref,
    packed_out, west_in, east_in, south_in, north_in, corner_in,
    obs_ref, innovation_ref, precision_ref, column_ref,
    landed, part_a, part_b, slots_a, slots_b,
    table, gram, upper, inverse, flat,
    packed_ref, south_edge, north_edge, corner_edge,
    send_near, recv_near, send_a, recv_a, send_b, recv_b, send_edge, recv_edge, packed_sem, input_sem,
):
    gx = lax.axis_index("gx")
    gy = lax.axis_index("gy")

    def device(dx, dy):
        return (lax.rem(gx + dx + NB, NB), lax.rem(gy + dy + NB, NB))

    barrier = pltpu.get_barrier_semaphore()
    peers = [(0, d) for d in range(1, NB)] + [(d, 0) for d in range(1, NB)]
    peers += [(1, 1), (1, -1), (-1, 1), (-1, -1)]
    for dx, dy in peers:
        pl.semaphore_signal(barrier, inc=1, device_id=device(dx, dy), device_id_type=MESH)

    inputs = [
        (obs_in, obs_ref),
        (innovation_in, innovation_ref),
        (precision_in, precision_ref),
        (column_in, column_ref),
    ]
    inputs = [
        pltpu.make_async_copy(src, dst, input_sem.at[n]) for n, (src, dst) in enumerate(inputs)
    ]
    for copy in inputs:
        copy.start()
    gram[...] = jnp.zeros_like(gram)
    table[...] = jnp.zeros_like(table)
    inverse[...] = jnp.zeros_like(inverse)
    for copy in inputs:
        copy.wait()
    centered = obs_ref[...].astype(F32)
    centered = centered - jnp.sum(centered, axis=0, keepdims=True) * (1.0 / M)
    innovation = innovation_ref[...]
    slot = lax.broadcasted_iota(jnp.int32, (1, SLOTS), 1)
    weight = jnp.where(slot < count_ref[0, 0], precision_ref[...], 0.0)
    column = column_ref[...]
    east = (gx * CX + lax.shift_right_logical(column, 5)).astype(F32) + 0.5
    north = (gy * CY + jnp.bitwise_and(column, 31)).astype(F32) + 0.5
    mine = landed.at[0]
    mine[0:M, :] = centered
    mine[M : M + 8, :] = jnp.concatenate(
        [innovation, weight, east, north, jnp.zeros((4, SLOTS), F32)], axis=0
    )
    numer = jnp.sum(weight * innovation * innovation, axis=1, keepdims=True)
    squares = jnp.sum(centered * centered, axis=0, keepdims=True)
    denom = jnp.sum(weight * squares, axis=1, keepdims=True) / (M - 1)
    lane = lax.broadcasted_iota(jnp.int32, (1, 128), 1)
    part = jnp.where(lane < 64, numer, denom)
    part_a[...] = part

    pl.semaphore_wait(barrier, len(peers))

    def spread(src, slots, send, recv, along_x):
        copies = []
        for d in range(1, NB):
            copy = pltpu.make_async_remote_copy(
                src_ref=src,
                dst_ref=slots.at[d],
                send_sem=send.at[d],
                recv_sem=recv.at[d],
                device_id=device(d, 0) if along_x else device(0, d),
                device_id_type=MESH,
            )
            copies.append(copy)
        return copies

    first = spread(part_a, slots_a, send_a, recv_a, False)
    for copy in first:
        copy.start()
    near = []
    for n, (dx, dy) in enumerate(NEIGHBOURS):
        copy = pltpu.make_async_remote_copy(
            src_ref=mine,
            dst_ref=landed.at[n + 1],
            send_sem=send_near.at[n],
            recv_sem=recv_near.at[n],
            device_id=device(dx, dy),
            device_id_type=MESH,
        )
        copy.start()
        near.append(copy)
    region = lax.broadcasted_iota(jnp.int32, (NREG, SLOTS), 0)
    centre_east = (gx * CX + 2 * lax.shift_right_logical(region, 4)).astype(F32) + 1.0
    centre_north = (gy * CY + 2 * jnp.bitwise_and(region, 15)).astype(F32) + 1.0

    def tile(t, carry):
        for n in range(8):

            @pl.when(t == n + 1)
            def arrive(copy=near[n]):
                copy.wait()

        @pl.when(t == 5)
        def relay():
            total = part_a[...]
            for copy in first:
                copy.wait()
            for d in range(1, NB):
                total = total + slots_a[d]
            part_b[...] = total
            for copy in spread(part_b, slots_b, send_b, recv_b, True):
                copy.start()

        obs = landed.at[t]
        east = obs[M + 2 : M + 3, :]
        north = obs[M + 3 : M + 4, :]
        weight = obs[M + 1 : M + 2, :]
        innovation = obs[M : M + 1, :]
        de = east - centre_east + 128.0
        de = jnp.where(de < 0.0, de + 256.0, de)
        de = jnp.where(de >= 256.0, de - 256.0, de) - 128.0
        dn = north - centre_north
        reach = jnp.maximum(1.0 - (de * de + dn * dn) * (1.0 / 256.0), 0.0)
        reach = reach * reach * weight
        reach_high, reach_low = split(reach)
        both = jnp.concatenate([reach_high, reach_low], axis=0)
        for b, (ib, jb) in enumerate(BLOCKS):
            right = obs[8 * jb : 8 * jb + 8, :]
            for ii in range(0, 8, 2):
                i = 8 * ib + ii
                rows = jnp.concatenate(
                    [obs[i : i + 1, :] * right, obs[i + 1 : i + 2, :] * right], axis=0
                )
                high, low = split(rows)
                at = b * 64 + ii * 8
                table[at : at + 16, :SLOTS] = high
                table[at : at + 16, SLOTS:] = low
        pull = jnp.concatenate([obs[0:M, :] * innovation, jnp.zeros((8, SLOTS), F32)], axis=0)
        high, low = split(pull)
        table[960:1008, :SLOTS] = high
        table[960:1008, SLOTS:] = low
        twice = jnp.concatenate([both, both], axis=1)
        for c in range(0, 1024, 256):
            out = lax.dot_general(
                table[c : c + 256, :], twice, (((1,), (1,)), ((), ())),
                preferred_element_type=F32,
            )
            gram[c : c + 256, :] += out[:, :128] + out[:, 128:]
        return carry

    lax.fori_loop(0, 9, tile, 0)

    lane = lax.broadcasted_iota(jnp.int32, (1, 128), 1)
    for copy in spread(part_b, slots_b, send_b, recv_b, True):
        copy.wait()
    both = part_b[...]
    for d in range(1, NB):
        both = both + slots_b[d]
    numer = jnp.sum(jnp.where(lane == 0, both, 0.0), axis=1, keepdims=True)
    denom = jnp.sum(jnp.where(lane == 64, both, 0.0), axis=1, keepdims=True)
    prior = jnp.broadcast_to((M - 1) / (numer / denom), (8, 128))
    sub = lax.broadcasted_iota(jnp.int32, (8, 128), 0)
    offset = {pair: 64 * b for b, pair in enumerate(BLOCKS)}

    for ib in range(5):
        cols = list(range(ib, 5))
        state = []
        for t in range(8):
            row = []
            for jb in cols:
                at = offset[(ib, jb)] + 8 * t
                value = gram[at : at + 8, :]
                if jb == ib:
                    value = value + jnp.where(sub == t, prior, 0.0)
                row.append(value)
            row += [jnp.zeros((8, 128), F32)] * ib
            state.append(row)

        def eliminate(p, state):
            base = p * M
            line = [upper[pl.ds(pl.multiple_of(base + 8 * jb, 8), 8), :] for jb in cols]
            line += [inverse[pl.ds(pl.multiple_of(base + 8 * jb, 8), 8), :] for jb in range(ib)]
            new = []
            for t in range(8):
                factor = upper[pl.ds(base + 8 * ib + t, 1), :]
                factor = jnp.broadcast_to(factor, (8, 128))
                new.append([s - factor * v for s, v in zip(state[t], line)])
            return new

        if ib:
            state = lax.fori_loop(0, 8 * ib, eliminate, state, unroll=4)
        state = [
            row + [jnp.where(sub == t, 1.0, 0.0).astype(F32)] for t, row in enumerate(state)
        ]
        for t in range(8):
            scale = lax.rsqrt(jnp.broadcast_to(state[t][0][t : t + 1, :], (8, 128)))
            state[t] = [v * scale for v in state[t]]
            for s in range(t + 1, 8):
                factor = jnp.broadcast_to(state[t][0][s : s + 1, :], (8, 128))
                state[s] = [a - factor * v for a, v in zip(state[s], state[t])]
            p = 8 * ib + t
            for jb, value in zip(cols, state[t][: len(cols)]):
                upper[p * M + 8 * jb : p * M + 8 * jb + 8, :] = value
            for jb, value in enumerate(state[t][len(cols) :]):
                inverse[p * M + 8 * jb : p * M + 8 * jb + 8, :] = value

    pull = [gram[960 + 8 * jb : 968 + 8 * jb, :] for jb in range(5)]
    mean = [jnp.zeros((8, 128), F32)] * 5
    sums = []
    for k in range(M):
        rows = [inverse[k * M + 8 * jb : k * M + 8 * jb + 8, :] for jb in range(k // 8 + 1)]
        inner = rows[0] * pull[0]
        plain = rows[0]
        for jb in range(1, len(rows)):
            inner = inner + rows[jb] * pull[jb]
            plain = plain + rows[jb]
        inner = jnp.broadcast_to(jnp.sum(inner, axis=0, keepdims=True), (8, 128))
        sums.append(jnp.broadcast_to(jnp.sum(plain, axis=0, keepdims=True), (8, 128)))
        for jb in range(len(rows)):
            mean[jb] = mean[jb] + rows[jb] * inner
    mean_sum = mean[0] + mean[1] + mean[2] + mean[3] + mean[4]
    mean_sum = jnp.broadcast_to(jnp.sum(mean_sum, axis=0, keepdims=True), (8, 128))
    root = math.sqrt(M - 1)
    for g in range(GROUPS):
        rows = []
        for part in range(3):
            k = part * GROUPS + g
            if k >= M:
                rows += [jnp.zeros((8, 128), F32)] * 5
                continue
            shift = (1.0 - mean_sum - root * sums[k]) * (1.0 / M)
            for jb in range(5):
                value = mean[jb] + shift
                if jb <= k // 8:
                    value = value + root * inverse[k * M + 8 * jb : k * M + 8 * jb + 8, :]
                rows.append(value)
        rows.append(jnp.zeros((8, 128), F32))
        turned = jnp.transpose(jnp.concatenate(rows, axis=0))
        packed_ref[g] = turned.reshape(RX, RY, 128)
        flat[g * NREG : (g + 1) * NREG, :] = turned
        south_edge[g] = flat[pl.ds(g * NREG, RX, stride=RY), :]
        north_edge[g] = flat[pl.ds(g * NREG + RY - 1, RX, stride=RY), :]
    flat[GROUPS * NREG : 16 * NREG, :] = jnp.zeros((2 * NREG, 128), F32)
    for c, r in enumerate((0, RY - 1, NREG - RY, NREG - 1)):
        corner_edge[c] = flat[pl.ds(r, 16, stride=NREG), :]

    plan = [
        (packed_ref.at[:, 0], east_in, (-1, 0)),
        (packed_ref.at[:, RX - 1], west_in, (1, 0)),
        (south_edge, north_in, (0, -1)),
        (north_edge, south_in, (0, 1)),
        (corner_edge.at[0], corner_in.at[3], (-1, -1)),
        (corner_edge.at[1], corner_in.at[2], (-1, 1)),
        (corner_edge.at[2], corner_in.at[1], (1, -1)),
        (corner_edge.at[3], corner_in.at[0], (1, 1)),
    ]
    copies = []
    for n, (src, dst, (dx, dy)) in enumerate(plan):
        copy = pltpu.make_async_remote_copy(
            src_ref=src,
            dst_ref=dst,
            send_sem=send_edge.at[n],
            recv_sem=recv_edge.at[n],
            device_id=device(dx, dy),
            device_id_type=MESH,
        )
        copy.start()
        copies.append(copy)
    leave = pltpu.make_async_copy(packed_ref, packed_out, packed_sem)
    leave.start()
    for copy in copies:
        copy.wait()
    leave.wait()


def analyse(obs, innovation, precision, column, count):
    shapes = [(GROUPS, RY, 128), (GROUPS, RY, 128), (GROUPS, RX, 128), (GROUPS, RX, 128), (4, 16, 128)]
    return pl.pallas_call(
        analyse_kernel,
        out_shape=tuple(jax.ShapeDtypeStruct(s, F32) for s in [(GROUPS, RX, RY, 128)] + shapes),
        in_specs=[pl.BlockSpec(memory_space=pl.ANY)] * 4 + [pl.BlockSpec(memory_space=pltpu.SMEM)],
        out_specs=(pl.BlockSpec(memory_space=pl.ANY),) * 6,
        scratch_shapes=[
            pltpu.VMEM((M, SLOTS), BF16),
            pltpu.VMEM((1, SLOTS), F32),
            pltpu.VMEM((1, SLOTS), F32),
            pltpu.VMEM((1, SLOTS), jnp.int32),
            pltpu.VMEM((9, ROWS, SLOTS), F32),
            pltpu.VMEM((1, 128), F32),
            pltpu.VMEM((1, 128), F32),
            pltpu.VMEM((NB, 1, 128), F32),
            pltpu.VMEM((NB, 1, 128), F32),
            pltpu.VMEM((1024, 2 * SLOTS), BF16),
            pltpu.VMEM((1024, NREG), F32),
            pltpu.VMEM((M * M, 128), F32),
            pltpu.VMEM((M * M, 128), F32),
            pltpu.VMEM((16 * NREG, 128), F32),
            pltpu.VMEM((GROUPS, RX, RY, 128), F32),
            pltpu.VMEM((GROUPS, RX, 128), F32),
            pltpu.VMEM((GROUPS, RX, 128), F32),
            pltpu.VMEM((4, 16, 128), F32),
            pltpu.SemaphoreType.DMA((8,)),
            pltpu.SemaphoreType.DMA((8,)),
            pltpu.SemaphoreType.DMA((NB,)),
            pltpu.SemaphoreType.DMA((NB,)),
            pltpu.SemaphoreType.DMA((NB,)),
            pltpu.SemaphoreType.DMA((NB,)),
            pltpu.SemaphoreType.DMA((8,)),
            pltpu.SemaphoreType.DMA((8,)),
            pltpu.SemaphoreType.DMA,
            pltpu.SemaphoreType.DMA((4,)),
        ],
        compiler_params=pltpu.CompilerParams(collective_id=0, has_side_effects=True),
        name="analyse",
    )(obs, innovation, precision, column, count)


def apply_kernel(
    state_ref, packed_ref, west_ref, east_ref, south_ref, north_ref, corner_ref,
    out_ref,
    frame, south, north, corner, state, after,
    weights_0, weights_1, members_0, members_1, results_0, results_1,
    frame_sem, read_sem, write_sem,
):
    weights = (weights_0, weights_1)
    members = (members_0, members_1)
    results = (results_0, results_1)

    def reads(a):
        return pltpu.make_async_copy(state_ref.at[:, a], state.at[a], read_sem.at[a])

    def writes(a):
        return pltpu.make_async_copy(after.at[a], out_ref.at[:, a], write_sem.at[a])

    reads(0).start()
    loads = [
        (packed_ref, frame.at[:, pl.ds(1, RX), pl.ds(8, RY)]),
        (west_ref, frame.at[:, 0, pl.ds(8, RY)]),
        (east_ref, frame.at[:, RX + 1, pl.ds(8, RY)]),
        (south_ref, south),
        (north_ref, north),
        (corner_ref, corner),
    ]
    loads = [
        pltpu.make_async_copy(src, dst, frame_sem.at[n]) for n, (src, dst) in enumerate(loads)
    ]
    for copy in loads:
        copy.start()
    for a in range(1, AHEAD):
        reads(a).start()

    def take(j, a, half):
        members[half][j * STRIDE : j * STRIDE + CY, :] = state[a, j].astype(F32)

    def blend(g, p, half):
        def east(start):
            near = frame[g, p + 1, start : start + 16, :]
            far = frame[g, p + 2 * half, start : start + 16, :]
            return 0.75 * near + 0.25 * far

        centre = 0.75 * east(8)
        weights[half][g * STRIDE : g * STRIDE + 16, :] = centre + 0.25 * east(7)
        weights[half][g * STRIDE + 16 : g * STRIDE + 32, :] = centre + 0.25 * east(9)

    def give(k, a, half):
        after[a, k] = results[half][k * STRIDE : k * STRIDE + CY, :].astype(BF16)

    lane = lax.broadcasted_iota(jnp.int32, (16, 128), 1)
    low_side = lane >= M

    def column(y, half):
        q, par = y // 2, y % 2
        block = members[half][pl.ds(y, M, stride=STRIDE), :].astype(BF16)
        block = jnp.concatenate([block, block], axis=0)
        value = weights[half][pl.ds(par * 16 + q, 16, stride=STRIDE), :]
        high = value.astype(BF16)
        low = (value - high.astype(F32)).astype(BF16)
        left = jnp.concatenate([
            jnp.where(low_side, pltpu.roll(low, 40, 1), high),
            jnp.where(low_side, low, pltpu.roll(high, 128 - 40, 1)),
            jnp.where(low_side, pltpu.roll(low, 128 - 40, 1), pltpu.roll(high, 128 - 80, 1)),
        ], axis=0)[:, : 2 * M]
        out = jnp.dot(left, block, preferred_element_type=F32)
        result = results[half]
        result[pl.ds(y, 14, stride=STRIDE), :] = out[0:14]
        result[pl.ds(14 * STRIDE + y, 14, stride=STRIDE), :] = out[16:30]
        result[pl.ds(28 * STRIDE + y, 12, stride=STRIDE), :] = out[32:44]

    reads(0).wait()
    for j in range(M):
        take(j, 0, 0)
    for copy in loads:
        copy.wait()
    gy = lax.axis_index("gy")
    bottom = gy == 0
    top = gy == NB - 1
    for g in range(GROUPS):
        for p in range(RX + 2):
            if p == 0:
                below, above = corner[0, g : g + 1], corner[1, g : g + 1]
            elif p == RX + 1:
                below, above = corner[2, g : g + 1], corner[3, g : g + 1]
            else:
                below, above = south[g, p - 1 : p], north[g, p - 1 : p]
            frame[g, p, 7:8, :] = jnp.where(bottom, frame[g, p, 8:9, :], below)
            frame[g, p, 24:25, :] = jnp.where(top, frame[g, p, 23:24, :], above)
    for g in range(GROUPS):
        blend(g, 0, 0)

    def pair(i, carry):
        for half in range(2):
            a = 2 * i + half
            later = jnp.minimum(a + 1, CX - 1)
            before = jnp.maximum(a - 1, 0)

            @pl.when(a + 1 < CX)
            def arrive():
                reads(later).wait()

            @pl.when(a + AHEAD < CX)
            def ahead():
                reads(jnp.minimum(a + AHEAD, CX - 1)).start()

            jobs = [functools.partial(give, k, before, 1 - half) for k in range(M)]
            jobs += [functools.partial(blend, g, lax.div(later, 2), 1 - half) for g in range(GROUPS)]
            jobs += [functools.partial(take, j, later, 1 - half) for j in range(M)]
            done = 0
            for y in range(CY):
                column(y, half)
                until = (y + 1) * len(jobs) // CY
                for job in jobs[done:until]:
                    job()
                done = until

            @pl.when(a > 0)
            def leave():
                writes(before).start()

        return carry

    lax.fori_loop(0, CX // 2, pair, 0)
    for k in range(M):
        give(k, CX - 1, 1)
    writes(CX - 1).start()
    for a in range(CX):
        writes(a).wait()


def apply(state, packed, west, east, south, north, corner):
    return pl.pallas_call(
        apply_kernel,
        out_shape=jax.ShapeDtypeStruct((M, CX, CY, 128), BF16),
        in_specs=[pl.BlockSpec(memory_space=pl.ANY)] * 7,
        out_specs=pl.BlockSpec(memory_space=pl.ANY),
        scratch_shapes=[
            pltpu.VMEM((GROUPS, RX + 2, 32, 128), F32),
            pltpu.VMEM((GROUPS, RX, 128), F32),
            pltpu.VMEM((GROUPS, RX, 128), F32),
            pltpu.VMEM((4, 16, 128), F32),
            pltpu.VMEM((CX, M, CY, 128), BF16),
            pltpu.VMEM((CX, M, CY, 128), BF16),
            pltpu.VMEM((16 * STRIDE, 128), F32),
            pltpu.VMEM((16 * STRIDE, 128), F32),
            pltpu.VMEM((M * STRIDE, 128), F32),
            pltpu.VMEM((M * STRIDE, 128), F32),
            pltpu.VMEM((M * STRIDE, 128), F32),
            pltpu.VMEM((M * STRIDE, 128), F32),
            pltpu.SemaphoreType.DMA((6,)),
            pltpu.SemaphoreType.DMA((CX,)),
            pltpu.SemaphoreType.DMA((CX,)),
        ],
        name="apply",
    )(state, packed, west, east, south, north, corner)


def per_device(background, obs_perturb, innovation, obs_precision, obs_column, obs_count):
    parts = analyse(
        obs_perturb[0, 0], innovation[0], obs_precision[0], obs_column[0], obs_count
    )
    return apply(background, *parts)


def solution(mesh):
    return jax.shard_map(
        per_device,
        mesh=mesh,
        in_specs=(
            P(None, "gx", "gy", None),
            P("gx", "gy", None, None),
            P("gx", "gy", None),
            P("gx", "gy", None),
            P("gx", "gy", None),
            P("gx", "gy"),
        ),
        out_specs=P(None, "gx", "gy", None),
        check_vma=False,
    )
```
